256 devices in a mesh: scen: 16 (over z, y_hi), gen: 16 (over y_lo, x, core).
Axes of the slice: x: 4, y: 4 (y_hi: 2, y_lo: 2; y = y_hi * 2 + y_lo), z: 8, core: 2. Of those that a mesh axis runs over, the one named last changes fastest.
Arguments:
- zone_load: float32 [256, 16, 256], P('scen'), may hold values from 0.3 to 1
- linear_cost: float32 [16, 20480], P(None, 'gen'), may hold values from -4 to 4
- cost_diag: float32 [20480], P('gen'), may hold values from 0.5 to 2
- capacity: float32 [20480], P('gen'), may hold values from 0.5 to 2
- cost_tiles: bfloat16 [80, 256, 256], P('gen'), may hold values from -0.375 to 0.375
- coupling_tiles: bfloat16 [16, 80, 256, 256], P('scen', 'gen'), may hold values from -0.375 to 0.375
- block_map: int32 [16, 80], P('scen', 'gen'), may hold values 0 or 1
- zone_index: int32 [20480], P('gen'), may hold values from 0 to 255
- step_numer: int32 [5], replicated, may hold values from 1 to 4
- step_denom: int32 [5], replicated, may hold values from 5 to 8
Outputs:
- dispatch: float32 [256, 16, 20480], P('scen', None, 'gen')
- prices: float32 [256, 16, 256], P('scen')
- plan: float32 [16, 20480], P(None, 'gen')
The draws below stay inside these ranges and needn't reach their ends.
All inputs are finite; a program needn't handle non-finite values. No bound on the sum of `block_map` on one device may be relied on, other than what follows from the above.
Results may differ from the reference program's by a relative error of at most 0.0003.
Values sent between devices are 32-bit elements; how exact they have to be, the bound alone decides.
A program may use at most 64 MiB of HBM per device.

```python
import math
import jax
import jax.numpy as jnp
from jax import lax

S_DEV = 16
P_SIZE = 16
G = 20480
TILE = 256
ZONES = 256
ITERS = 5
S = 256
GB = 80
SBLOCKS = 16


def plant(result, key, low, top_value):
    dims = result.shape
    place = [jax.random.randint(jax.random.fold_in(key, axis), (), 0, dims[axis]) for axis in range(len(dims))]
    result = result.at[tuple(place)].set(low)
    longest = dims.index(max(dims))
    place[longest] = (place[longest] + 1) % dims[longest]
    return result.at[tuple(place)].set(top_value)


def level_of(rng, shape, pieces, smallest, largest):
    level = 1.0
    for position, shards_of in pieces:
        draws = jax.random.uniform(jax.random.fold_in(jax.random.fold_in(rng, 6), position), (shards_of,), jnp.float32, smallest / len(pieces), largest / len(pieces))
        level = level * jnp.repeat(jnp.exp(draws), shape[position] // shards_of).reshape((-1,) + (1,) * (len(shape) - 1 - position))
    return level


def bell_draw(stream_key, extent, scale, bound, shards=(), kind=jnp.bfloat16):
    values = scale * jax.random.normal(stream_key, extent, jnp.float32)
    if shards:
        values = values * level_of(stream_key, extent, shards, -0.22, 0.18)
    return jnp.clip(values, -bound, bound).astype(kind)


def setup_inputs(seed: int = 0) -> dict:
    seeds = jax.random.split(jax.random.key(seed), 11)
    zone_load = jnp.clip(0.3 + 0.7 * jax.random.uniform(seeds[0], (S, P_SIZE, ZONES), jnp.float32) ** level_of(seeds[0], (S, P_SIZE, ZONES), ((0, 16),), -0.2, 0.2), 0.3, 1.0)
    linear_cost = bell_draw(seeds[1], (P_SIZE, G), 1.0, 4.0, ((1, 16),), jnp.float32)
    cost_diag = jnp.clip(jnp.exp(math.log(2.0) - 1.3862944 * jax.random.uniform(seeds[2], (G,), jnp.float32) ** level_of(seeds[2], (G,), ((0, 16),), -0.2, 0.2)), 0.5, 2.0)
    capacity = jnp.clip(jnp.exp(math.log(2.0) - 1.3862944 * jax.random.uniform(seeds[3], (G,), jnp.float32) ** level_of(seeds[3], (G,), ((0, 16),), -0.2, 0.2)), 0.5, 2.0)
    cost_tiles = bell_draw(seeds[4], (GB, TILE, TILE), TILE ** -0.5, 0.375, ((0, 16),))
    coupling_tiles = bell_draw(seeds[5], (SBLOCKS, GB, TILE, TILE), TILE ** -0.5, 0.375, ((0, 16), (1, 16)))
    block_map = plant((jax.random.randint(seeds[6], (SBLOCKS, GB), 0, 2) < 1).astype(jnp.int32), jax.random.fold_in(seeds[6], 1), 0, 1)
    zone_index = plant(jax.random.randint(seeds[7], (G,), 0, ZONES), jax.random.fold_in(seeds[7], 1), 0, ZONES - 1).astype(jnp.int32)
    step_numer = plant(jax.random.randint(seeds[8], (ITERS,), 1, 5), jax.random.fold_in(seeds[8], 1), 1, 4).astype(jnp.int32)
    step_denom = plant(jax.random.randint(seeds[9], (ITERS,), 5, 9), jax.random.fold_in(seeds[9], 1), 5, 8).astype(jnp.int32)
    return dict(zone_load=zone_load, linear_cost=linear_cost, cost_diag=cost_diag, capacity=capacity, cost_tiles=cost_tiles, coupling_tiles=coupling_tiles, block_map=block_map, zone_index=zone_index, step_numer=step_numer, step_denom=step_denom)


penalty = 2.0
centering = 0.5
epsilon = 1e-06

def tile_products(dispatch_block, cost_tiles, coupling, block_mask):
    rounded = lax.optimization_barrier(dispatch_block.astype(jnp.bfloat16))
    row_data = rounded.reshape(S_DEV * P_SIZE, GB, TILE).astype(jnp.float32)
    own_part = jnp.einsum('rki,kij->rkj', row_data, cost_tiles.astype(jnp.float32))
    cross_part = jnp.einsum('rki,kij->rkj', row_data, coupling.astype(jnp.float32))
    combined = own_part + cross_part * block_mask.astype(jnp.float32)[None, :, None]
    return combined.reshape(S_DEV, P_SIZE, G)

def reference(zone_load, linear_cost, cost_diag, capacity, cost_tiles, coupling_tiles, block_map, zone_index, step_numer, step_denom):
    blocks = S // S_DEV
    levels = 0.2 + 0.6 * (jnp.arange(S, dtype=jnp.float32) + 0.5) / S
    dispatch = (levels.reshape(blocks, S_DEV, 1, 1) * capacity).astype(jnp.float32)
    dispatch = jnp.broadcast_to(dispatch, (blocks, S_DEV, P_SIZE, G))
    low_dual = jnp.ones((blocks, S_DEV, P_SIZE, G), jnp.float32)
    high_dual = jnp.ones((blocks, S_DEV, P_SIZE, G), jnp.float32)
    prices = jnp.zeros((S, P_SIZE, ZONES), jnp.float32)
    lowest = 0.02 * capacity
    highest = 0.98 * capacity
    plan = jnp.zeros((P_SIZE, G), jnp.float32)
    for iteration in range(ITERS):
        step_size = step_numer[iteration].astype(jnp.float32) / step_denom[iteration].astype(jnp.float32)
        plan = lax.optimization_barrier(jnp.sum(dispatch, axis=(0, 1))) / S
        flattened = dispatch.reshape(S * P_SIZE, G)
        totals = jnp.zeros((S * P_SIZE, ZONES), jnp.float32).at[:, zone_index].add(flattened)
        imbalance = totals.reshape(S, P_SIZE, ZONES) * (ZONES / G) - zone_load
        price_blocks = prices.reshape(blocks, S_DEV, P_SIZE, ZONES)

        def residual_block(inputs):
            dispatch_block, low_block, high_block, price_block, coupling, block_mask = inputs
            products = tile_products(dispatch_block, cost_tiles, coupling, block_mask)
            return cost_diag * dispatch_block + products + linear_cost + penalty * (dispatch_block - plan) + price_block[..., zone_index] - low_block + high_block
        residual = lax.map(residual_block, (dispatch, low_dual, high_dual, price_blocks, coupling_tiles, block_map))
        gap_sum = jnp.sum(dispatch * low_dual + (capacity - dispatch) * high_dual)
        dual_sq = jnp.sum(residual * residual)
        primal_sq = jnp.sum(imbalance * imbalance)
        target = centering * gap_sum / (2.0 * S * P_SIZE * G)
        dual_rms = jnp.sqrt(dual_sq / (S * P_SIZE * G) + epsilon)
        primal_rms = jnp.sqrt(primal_sq / (S * P_SIZE * ZONES) + epsilon)
        scaling = cost_diag + penalty + low_dual / dispatch + high_dual / (capacity - dispatch)
        updated = jnp.clip(dispatch - step_size * residual / (scaling * (1.0 + dual_rms)), lowest, highest)
        low_dual = low_dual + step_size * (target / updated - low_dual)
        high_dual = high_dual + step_size * (target / (capacity - updated) - high_dual)
        prices = prices + step_size * imbalance / (1.0 + primal_rms)
        dispatch = updated
    return (dispatch.reshape(S, P_SIZE, G), prices, plan)
```

```python
import functools
import itertools

import jax
import jax.numpy as jnp
from jax import lax
from jax.experimental import pallas as pl
from jax.experimental.pallas import tpu as pltpu
from jax.sharding import PartitionSpec as P

ITERS = 5
MESH = pl.DeviceIdType.MESH
F32 = jnp.float32
BF16 = jnp.bfloat16
LANES = 128

penalty = 2.0
centering = 0.5
epsilon = 1e-06


def ring_hops(offset, size):
    return min(offset, size - offset)


def partners(dims, weights):
    result = []
    for offset in itertools.product(*[range(n) for n in dims]):
        if not any(offset):
            continue
        hops = sum(w * ring_hops(o, n) for o, n, w in zip(offset, dims, weights))
        back = 0
        for o, n in zip(offset, dims):
            back = back * n + (n - o) % n
        result.append((hops, offset, back - 1))
    result.sort(key=lambda item: -item[0])
    return [(offset, slot) for _, offset, slot in result]


def member(me, dims, offset):
    index = 0
    stride = 1
    for n, o in zip(reversed(dims), reversed(offset)):
        coordinate = (me // stride) % n
        index = index + ((coordinate + o) % n) * stride
        stride *= n
    return index


def kernel(
    scen_dims,
    gen_dims,
    entries,
    zone_entries,
    zone_scale,
    load_ref,
    linear_ref,
    diag_ref,
    cap_ref,
    cost_ref,
    coupling_ref,
    map_ref,
    zone_ref,
    numer_ref,
    denom_ref,
    x_ref,
    prices_ref,
    plan_ref,
    low_ref,
    high_ref,
    res_ref,
    inv_ref,
    onehot_ref,
    masked_ref,
    xb_ref,
    zp_ref,
    zr_ref,
    cs_ref,
    cr_ref,
    ts_ref,
    tr_ref,
    pg_ref,
    imb_ref,
    us_ref,
    ur_ref,
    send_sem,
    recv_sem,
):
    me_s = lax.axis_index("scen")
    me_g = lax.axis_index("gen")
    n_s = 1
    for n in scen_dims:
        n_s *= n
    n_g = 1
    for n in gen_dims:
        n_g *= n
    scen_partners = [
        (member(me_s, scen_dims, offset), slot)
        for offset, slot in partners(scen_dims, (1,) + (2,) * (len(scen_dims) - 1))
    ]
    gen_partners = [
        (member(me_g, gen_dims, offset), slot)
        for offset, slot in partners(gen_dims, (2,) * (len(gen_dims) - 1) + (1,))
    ]

    barrier = pltpu.get_barrier_semaphore()
    for target, _ in scen_partners:
        pl.semaphore_signal(barrier, inc=1, device_id={"scen": target}, device_id_type=MESH)
    for target, _ in gen_partners:
        pl.semaphore_signal(barrier, inc=1, device_id={"gen": target}, device_id_type=MESH)

    rows, width = x_ref.shape
    periods = linear_ref.shape[0]
    scens = rows // periods
    zones = zp_ref.shape[1]
    blocks, tile, _ = cost_ref.shape
    tiles = tile // LANES
    lane_tiles = width // LANES
    halves = periods // 8
    group = cs_ref.shape[0] // periods
    share = rows // n_g
    plan_rows = pg_ref.shape[0] // n_s
    total_scen = scens * n_s

    def columns(j):
        return pl.ds(j * tile, tile)

    def scen_rows(s):
        return pl.ds(pl.multiple_of(s * periods, periods), periods)

    for j in range(blocks):
        zone_row = zone_ref[:, columns(j)]
        ids = lax.broadcasted_iota(jnp.int32, (zones, tile), 0)
        onehot_ref[:, columns(j)] = jnp.where(ids == zone_row, 1.0, 0.0).astype(BF16)
        mask = map_ref[0, j].astype(F32)
        masked_ref[j] = (coupling_ref[j].astype(F32) * mask).astype(BF16)

    def begin(s, carry):
        ids = jnp.full((periods, width), me_s * scens + s, jnp.int32)
        level = 0.2 + 0.6 * (ids.astype(F32) + 0.5) / total_scen
        x_ref[scen_rows(s), :] = level * cap_ref[...]
        low_ref[scen_rows(s), :] = jnp.ones((periods, width), F32)
        high_ref[scen_rows(s), :] = jnp.ones((periods, width), F32)
        return carry

    lax.fori_loop(0, scens, begin, 0)
    prices_ref[...] = jnp.zeros_like(prices_ref)
    cs_ref[...] = jnp.zeros_like(cs_ref)
    ts_ref[...] = jnp.zeros_like(ts_ref)
    us_ref[...] = jnp.zeros_like(us_ref)
    pg_ref[...] = jnp.zeros_like(pg_ref)

    pl.semaphore_wait(barrier, len(scen_partners) + len(gen_partners))

    def scen_send(kind, source, landing):
        for target, slot in scen_partners:
            pltpu.make_async_remote_copy(
                src_ref=source(target),
                dst_ref=landing(slot),
                send_sem=send_sem.at[kind],
                recv_sem=recv_sem.at[kind],
                device_id={"scen": target},
                device_id_type=MESH,
            ).start()

    def gen_send(kind, source, landing):
        for target, slot in gen_partners:
            pltpu.make_async_remote_copy(
                src_ref=source(target),
                dst_ref=landing(slot),
                send_sem=send_sem.at[kind],
                recv_sem=recv_sem.at[kind],
                device_id={"gen": target},
                device_id_type=MESH,
            ).start()

    def wait_for(sem, span):
        pltpu.make_async_copy(span, span, sem).wait()

    ZONE, COLUMN, TERM, PLAN, IMB, ALL = range(6)
    spans = {
        ZONE: zr_ref,
        COLUMN: cr_ref,
        TERM: tr_ref,
        PLAN: pg_ref.at[pl.ds(0, (n_s - 1) * plan_rows)],
        IMB: imb_ref.at[pl.ds(0, (n_g - 1) * share)],
        ALL: ur_ref,
    }

    def iteration(k, carry):
        step = jnp.full((1, 1), numer_ref[k], jnp.int32).astype(F32) / jnp.full(
            (1, 1), denom_ref[k], jnp.int32
        ).astype(F32)

        for j in range(blocks):
            value = x_ref[:, columns(j)]
            high_part = value.astype(BF16)
            low_part = (value - high_part.astype(F32)).astype(BF16)
            xb_ref[:, columns(j)] = high_part
            onehot = onehot_ref[:, columns(j)]
            contract = (((1,), (1,)), ((), ()))
            found = lax.dot_general(
                high_part, onehot, contract, preferred_element_type=F32
            ) + lax.dot_general(low_part, onehot, contract, preferred_element_type=F32)
            if j == 0:
                zp_ref[...] = found
            else:
                zp_ref[...] += found
        gen_send(
            ZONE,
            lambda t: zp_ref.at[pl.ds(t * share, share)],
            lambda slot: zr_ref.at[pl.ds(slot * share, share)],
        )

        price = prices_ref[...]
        price_high = price.astype(BF16)
        price_low = (price - price_high.astype(F32)).astype(BF16)
        gap_row = jnp.zeros((1, LANES), F32)
        square_row = jnp.zeros((1, LANES), F32)
        for j in range(blocks):
            left = xb_ref[:, columns(j)]
            onehot = onehot_ref[:, columns(j)]
            res_ref[:, columns(j)] = (
                jnp.dot(left, cost_ref[j], preferred_element_type=F32)
                + jnp.dot(left, masked_ref[j], preferred_element_type=F32)
                + jnp.dot(price_high, onehot, preferred_element_type=F32)
                + jnp.dot(price_low, onehot, preferred_element_type=F32)
            )
            diag = diag_ref[:, columns(j)]
            cap = cap_ref[:, columns(j)]
            linear = linear_ref[:, columns(j)]

            def part(s, sums):
                column, rest, gap, square = sums
                here = (scen_rows(s), columns(j))
                value = x_ref[here]
                low = low_ref[here]
                high = high_ref[here]
                residual = res_ref[here] + (diag + penalty) * value + linear - low + high
                res_ref[here] = residual
                gap = gap + (value * low + (cap - value) * high)
                return column + value, rest + residual, gap, square + residual * residual

            zero = jnp.zeros((periods, tile), F32)
            column, rest, gap, square = lax.fori_loop(
                0, scens, part, (zero, zero, zero, zero), unroll=2
            )
            for t in range(tiles):
                lanes = slice(t * LANES, (t + 1) * LANES)
                gap_row = gap_row + jnp.sum(gap[:, lanes], axis=0, keepdims=True)
                square_row = square_row + jnp.sum(square[:, lanes], axis=0, keepdims=True)
                for h in range(halves):
                    first = h * 8 * group + j * tiles + t
                    cs_ref[pl.ds(first, 8, stride=group), :] = column[h * 8 : h * 8 + 8, lanes]
                    cs_ref[pl.ds(first + lane_tiles, 8, stride=group), :] = rest[
                        h * 8 : h * 8 + 8, lanes
                    ]
        for h in range(halves):
            first = h * 8 * group + 2 * lane_tiles
            cs_ref[pl.ds(first, 8, stride=group), :] = jnp.broadcast_to(gap_row, (8, LANES))
            cs_ref[pl.ds(first + 1, 8, stride=group), :] = jnp.broadcast_to(square_row, (8, LANES))
        scen_send(
            COLUMN,
            lambda t: cs_ref.at[pl.ds(t * group, group)],
            lambda slot: cr_ref.at[pl.ds(slot * group, group)],
        )

        mine = pl.ds(pl.multiple_of(me_g * share, share), share)
        wait_for(recv_sem.at[ZONE], spans[ZONE])
        total = zp_ref[mine, :]
        for slot in range(n_g - 1):
            total = total + zr_ref[slot * share : (slot + 1) * share, :]
        imbalance = total * zone_scale - load_ref[mine, :]
        imb_ref[mine, :] = imbalance
        primal = jnp.sum(imbalance * imbalance, axis=0, keepdims=True)
        primal_row = jnp.zeros((1, LANES), F32)
        for t in range(zones // LANES):
            primal_row = primal_row + primal[:, t * LANES : (t + 1) * LANES]
        gen_send(
            IMB,
            lambda t: imb_ref.at[mine],
            lambda slot: imb_ref.at[mine],
        )

        wait_for(recv_sem.at[COLUMN], spans[COLUMN])
        sums = cs_ref[pl.ds(pl.multiple_of(me_s * group, 8), group), :]
        for slot in range(n_s - 1):
            sums = sums + cr_ref[slot * group : (slot + 1) * group, :]
        plan = sums[:lane_tiles] / total_scen
        rest = sums[lane_tiles : 2 * lane_tiles]
        term = (2.0 * penalty) * plan * ((penalty / 2.0) * total_scen * plan - rest)
        term_row = jnp.sum(term, axis=0, keepdims=True)
        gap_row = sums[2 * lane_tiles : 2 * lane_tiles + 1]
        square_row = sums[2 * lane_tiles + 1 : 2 * lane_tiles + 2]
        own = pl.multiple_of(me_s * plan_rows, plan_rows)
        ts_ref[0:1, :] = term_row
        ts_ref[1:2, :] = primal_row
        scen_send(
            TERM,
            lambda t: ts_ref,
            lambda slot: tr_ref.at[pl.ds(slot * 8, 8)],
        )
        pg_ref[pl.ds(own, lane_tiles), :] = plan
        scen_send(
            PLAN,
            lambda t: pg_ref.at[pl.ds(own, plan_rows)],
            lambda slot: pg_ref.at[pl.ds(own, plan_rows)],
        )

        for j in range(blocks):
            diag = diag_ref[:, columns(j)]
            cap = cap_ref[:, columns(j)]

            def scale(s, none):
                here = (scen_rows(s), columns(j))
                value = x_ref[here]
                scaling = (
                    diag + penalty + low_ref[here] / value + high_ref[here] / (cap - value)
                )
                inv_ref[here] = step / scaling
                return none

            lax.fori_loop(0, scens, scale, 0, unroll=2)

        wait_for(recv_sem.at[TERM], spans[TERM])
        both = ts_ref[...]
        for slot in range(n_s - 1):
            both = both + tr_ref[slot * 8 : (slot + 1) * 8, :]
        us_ref[0:1, :] = both[0:1] + square_row
        us_ref[1:2, :] = both[1:2]
        us_ref[2:3, :] = gap_row
        gen_send(
            ALL,
            lambda t: us_ref,
            lambda slot: ur_ref.at[pl.ds(slot * 8, 8)],
        )
        wait_for(recv_sem.at[PLAN], spans[PLAN])
        for j in range(blocks):
            pieces = [
                jnp.concatenate(
                    [
                        pg_ref[
                            pl.ds(h * 8 * plan_rows + j * tiles + t, 8, stride=plan_rows), :
                        ]
                        for t in range(tiles)
                    ],
                    axis=1,
                )
                for h in range(halves)
            ]
            plan_ref[:, columns(j)] = jnp.concatenate(pieces, axis=0)
        wait_for(recv_sem.at[IMB], spans[IMB])
        wait_for(recv_sem.at[ALL], spans[ALL])
        every = us_ref[...]
        for slot in range(n_g - 1):
            every = every + ur_ref[slot * 8 : (slot + 1) * 8, :]
        every = jnp.sum(every, axis=1, keepdims=True)
        dual_rms = jnp.sqrt(every[0:1] / entries + epsilon)
        primal_rms = jnp.sqrt(every[1:2] / zone_entries + epsilon)
        target = centering * every[2:3] / (2.0 * entries)
        shrink = 1.0 / (1.0 + dual_rms)
        prices_ref[...] += (step / (1.0 + primal_rms)) * imb_ref[...]

        for j in range(blocks):
            cap = cap_ref[:, columns(j)]
            lowest = 0.02 * cap
            highest = 0.98 * cap
            twice = penalty * plan_ref[:, columns(j)]

            def update(s, none):
                here = (scen_rows(s), columns(j))
                low = low_ref[here]
                high = high_ref[here]
                move = (res_ref[here] - twice) * inv_ref[here] * shrink
                value = jnp.clip(x_ref[here] - move, lowest, highest)
                x_ref[here] = value
                low_ref[here] = low + step * (target / value - low)
                high_ref[here] = high + step * (target / (cap - value) - high)
                return none

            lax.fori_loop(0, scens, update, 0, unroll=2)

        for kind, span in spans.items():
            wait_for(send_sem.at[kind], span)
        return carry

    lax.fori_loop(0, ITERS, iteration, 0)


def solution(mesh):
    n_s, n_g = mesh.shape["scen"], mesh.shape["gen"]
    scen_dims = (n_s // 2, 2)
    gen_dims = (2, n_g // 4, 2) if n_g >= 4 else (n_g,)

    def local(
        zone_load,
        linear_cost,
        cost_diag,
        capacity,
        cost_tiles,
        coupling_tiles,
        block_map,
        zone_index,
        step_numer,
        step_denom,
    ):
        scens, periods, zones = zone_load.shape
        width = capacity.shape[0]
        blocks, tile, _ = cost_tiles.shape
        rows = scens * periods
        lane_tiles = width // LANES
        group = -(-(2 * lane_tiles + 2) // 8) * 8
        plan_rows = -(-lane_tiles // 8) * 8
        entries = float(n_s * rows * width * n_g)
        zone_entries = float(n_s * rows * zones)
        vmem = pl.BlockSpec(memory_space=pltpu.VMEM)
        smem = pl.BlockSpec(memory_space=pltpu.SMEM)
        state = pltpu.VMEM((rows, width), F32)
        share = rows // n_g
        dispatch, prices, plan = pl.pallas_call(
            functools.partial(
                kernel,
                scen_dims,
                gen_dims,
                entries,
                zone_entries,
                zones / (width * n_g),
            ),
            out_shape=(
                jax.ShapeDtypeStruct((rows, width), F32),
                jax.ShapeDtypeStruct((rows, zones), F32),
                jax.ShapeDtypeStruct((periods, width), F32),
            ),
            in_specs=[vmem] * 6 + [smem, vmem, smem, smem],
            out_specs=(vmem, vmem, vmem),
            scratch_shapes=[
                state,
                state,
                state,
                state,
                pltpu.VMEM((zones, width), BF16),
                pltpu.VMEM((blocks, tile, tile), BF16),
                pltpu.VMEM((rows, width), BF16),
                pltpu.VMEM((rows, zones), F32),
                pltpu.VMEM(((n_g - 1) * share, zones), F32),
                pltpu.VMEM((periods * group, LANES), F32),
                pltpu.VMEM(((n_s - 1) * group, LANES), F32),
                pltpu.VMEM((8, LANES), F32),
                pltpu.VMEM(((n_s - 1) * 8, LANES), F32),
                pltpu.VMEM((n_s * plan_rows, LANES), F32),
                pltpu.VMEM((rows, zones), F32),
                pltpu.VMEM((8, LANES), F32),
                pltpu.VMEM(((n_g - 1) * 8, LANES), F32),
                pltpu.SemaphoreType.DMA((6,)),
                pltpu.SemaphoreType.DMA((6,)),
            ],
            compiler_params=pltpu.CompilerParams(collective_id=0, has_side_effects=True),
        )(
            zone_load.reshape(rows, zones),
            linear_cost,
            cost_diag.reshape(1, width),
            capacity.reshape(1, width),
            cost_tiles,
            coupling_tiles[0],
            block_map,
            zone_index.reshape(1, width),
            step_numer,
            step_denom,
        )
        return dispatch.reshape(scens, periods, width), prices.reshape(scens, periods, zones), plan

    return jax.shard_map(
        local,
        mesh=mesh,
        in_specs=(
            P("scen", None, None),
            P(None, "gen"),
            P("gen"),
            P("gen"),
            P("gen", None, None),
            P("scen", "gen", None, None),
            P("scen", "gen"),
            P("gen"),
            P(),
            P(),
        ),
        out_specs=(P("scen", None, "gen"), P("scen", None, None), P(None, "gen")),
        check_vma=False,
    )
```

```python
import functools
import itertools

import jax
import jax.numpy as jnp
from jax import lax
from jax.experimental import pallas as pl
from jax.experimental.pallas import tpu as pltpu
from jax.sharding import PartitionSpec as P

ITERS = 5
MESH = pl.DeviceIdType.MESH
F32 = jnp.float32
BF16 = jnp.bfloat16
LANES = 128

penalty = 2.0
centering = 0.5
epsilon = 1e-06


def ring(offset, size):
    return min(offset, size - offset)


def partners(dims, hops):
    result = []
    for offset in itertools.product(*[range(n) for n in dims]):
        if not any(offset):
            continue
        back = 0
        for o, n in zip(offset, dims):
            back = back * n + (n - o) % n
        result.append((hops(offset), offset, back - 1))
    result.sort(key=lambda item: -item[0])
    return [(offset, slot) for _, offset, slot in result]


def moved(me, dims, offset):
    index = 0
    stride = 1
    for n, o in zip(reversed(dims), reversed(offset)):
        coordinate = (me // stride) % n
        index = index + ((coordinate + o) % n) * stride
        stride *= n
    return index


def two_parts(value):
    high = value.astype(BF16)
    return high, (value - high.astype(F32)).astype(BF16)


def kernel(
    scen_dims,
    gen_dims,
    entries,
    zone_entries,
    zone_scale,
    load_ref,
    linear_ref,
    diag_in,
    cap_in,
    cost_ref,
    coupling_ref,
    map_ref,
    zone_in,
    numer_ref,
    denom_ref,
    x_ref,
    prices_ref,
    plan_ref,
    low_ref,
    high_ref,
    res_ref,
    inv_ref,
    onehot_ref,
    turned_ref,
    masked_ref,
    diag_ref,
    cap_ref,
    column_ref,
    round_ref,
    dual_ref,
    paid_ref,
    more_ref,
    zc_ref,
    zp_ref,
    zr_ref,
    cs_ref,
    cr_ref,
    pg_ref,
    imb_ref,
    ns_ref,
    nr_ref,
    fs_ref,
    fr_ref,
    all_ref,
    send_sem,
    recv_sem,
    far_sem,
):
    me_s = lax.axis_index("scen")
    me_g = lax.axis_index("gen")
    depth, sides = scen_dims
    n_s = depth * sides
    n_g = gen_dims[0] * gen_dims[1] * gen_dims[2]
    y_hops = {(0, 0): 0, (0, 1): 1, (1, 0): 2, (1, 1): 1}

    def scen_device(offset):
        return {"scen": moved(me_s, scen_dims, offset)}

    def gen_device(offset):
        return {"gen": moved(me_g, gen_dims, offset)}

    def plane_device(offset):
        return {
            "scen": moved(me_s, scen_dims, (0, offset[0])),
            "gen": moved(me_g, gen_dims, offset[1:]),
        }

    scen_group = partners(scen_dims, lambda o: ring(o[0], depth) + 2 * o[1])
    gen_group = partners(gen_dims, lambda o: 2 * o[0] + 2 * ring(o[1], gen_dims[1]) + o[2])
    line_group = partners((depth,), lambda o: ring(o[0], depth))
    plane_group = partners(
        (sides,) + gen_dims,
        lambda o: 2 * y_hops[o[:2]] + 2 * ring(o[2], gen_dims[1]) + o[3],
    )
    scen_to = [(scen_device(o), moved(me_s, scen_dims, o), slot) for o, slot in scen_group]
    gen_to = [(gen_device(o), moved(me_g, gen_dims, o), slot) for o, slot in gen_group]
    line_to = [(scen_device((o[0], 0)), 0, slot) for o, slot in line_group]
    plane_to = [(plane_device(o), 0, slot) for o, slot in plane_group]

    barrier = pltpu.get_barrier_semaphore()
    greeted = [device for device, _, _ in scen_to]
    greeted += [plane_device(o) for o, _ in plane_group if any(o[1:])]
    for device in greeted:
        pl.semaphore_signal(barrier, inc=1, device_id=device, device_id_type=MESH)

    rows, width = x_ref.shape
    periods = linear_ref.shape[0]
    scens = rows // periods
    zones = zp_ref.shape[1]
    blocks, tile, _ = cost_ref.shape
    tiles = tile // LANES
    lane_tiles = width // LANES
    halves = periods // 8
    group = cs_ref.shape[0] // periods
    share = rows // n_g
    plan_rows = pg_ref.shape[0] // n_s
    total_scen = scens * n_s
    mine = pl.ds(pl.multiple_of(me_g * share, share), share)
    own = pl.multiple_of(me_s * plan_rows, plan_rows)

    def columns(j):
        return pl.ds(j * tile, tile)

    def scen_rows(s):
        return pl.ds(pl.multiple_of(s * periods, periods), periods)

    def send(kind, to, source, landing, sem=None):
        for device, member, slot in to:
            pltpu.make_async_remote_copy(
                src_ref=source(member),
                dst_ref=landing(slot),
                send_sem=send_sem.at[kind],
                recv_sem=recv_sem.at[kind] if sem is None else sem,
                device_id=device,
                device_id_type=MESH,
            ).start()

    def wait_for(sem, span):
        pltpu.make_async_copy(span, span, sem).wait()

    ZONE, COLUMN, PLAN, IMB, NEAR, FAR, START = range(7)
    spans = {
        ZONE: zr_ref,
        COLUMN: cr_ref,
        PLAN: pg_ref.at[pl.ds(0, (n_s - 1) * plan_rows)],
        IMB: imb_ref.at[pl.ds(0, (n_g - 1) * share)],
        NEAR: nr_ref,
        FAR: fr_ref.at[0],
        START: zc_ref.at[pl.ds(0, n_g - 1)],
    }

    def level(s, shape):
        ids = jnp.full(shape, me_s * scens + s, jnp.int32)
        return 0.2 + 0.6 * (ids.astype(F32) + 0.5) / total_scen

    def step_of(k):
        numer = jnp.full((1, 1), numer_ref[k], jnp.int32).astype(F32)
        return numer / jnp.full((1, 1), denom_ref[k], jnp.int32).astype(F32)

    def fold(value):
        row = jnp.sum(value, axis=0, keepdims=True)
        return sum(row[:, t * LANES : (t + 1) * LANES] for t in range(value.shape[1] // LANES))

    diag_ref[...] = diag_in[...].reshape(1, width)
    cap_ref[...] = cap_in[...].reshape(1, width)
    zone_row = zone_in[...].reshape(1, width)
    start = jnp.zeros((16, zones), F32)
    for j in range(blocks):
        ids = lax.broadcasted_iota(jnp.int32, (zones, tile), 0)
        onehot = jnp.where(ids == zone_row[:, j * tile : (j + 1) * tile], 1.0, 0.0)
        onehot_ref[:, columns(j)] = onehot.astype(BF16)
        turned = onehot.T.astype(BF16)
        turned_ref[columns(j), :] = turned
        cap_high, cap_low = two_parts(jnp.broadcast_to(cap_ref[:, columns(j)], (8, tile)))
        both = jnp.concatenate([cap_high, cap_low], axis=0)
        start = start + jnp.dot(both, turned, preferred_element_type=F32)
    zc_ref[me_g] = start[0:1] + start[8:9]

    pl.semaphore_wait(barrier, len(greeted))
    send(START, gen_to, lambda t: zc_ref.at[me_g], lambda slot: zc_ref.at[me_g])

    for j in range(blocks):
        mask = map_ref[0, j].astype(F32)
        masked_ref[j] = (coupling_ref[j].astype(F32) * mask).astype(BF16)

    def begin(s, carry):
        here = scen_rows(s)
        x_ref[here, :] = level(s, (periods, width)) * cap_ref[...]
        low_ref[here, :] = jnp.ones((periods, width), F32)
        high_ref[here, :] = jnp.ones((periods, width), F32)
        return carry

    lax.fori_loop(0, scens, begin, 0, unroll=2)
    prices_ref[...] = jnp.zeros_like(prices_ref)
    paid_ref[...] = jnp.zeros_like(paid_ref)
    cs_ref[...] = jnp.zeros_like(cs_ref)
    ns_ref[...] = jnp.zeros_like(ns_ref)
    pg_ref[...] = jnp.zeros_like(pg_ref)

    def residuals(step, first):
        if not first:
            price_high, price_low = two_parts(prices_ref[...])
        gap_row = jnp.zeros((1, LANES), F32)
        square_row = jnp.zeros((1, LANES), F32)
        keep = 1.0 - step
        for j in range(blocks):
            left = x_ref[:, columns(j)].astype(BF16)
            found = jnp.dot(left, cost_ref[j], preferred_element_type=F32) + jnp.dot(
                left, masked_ref[j], preferred_element_type=F32
            )
            if not first:
                onehot = onehot_ref[:, columns(j)]
                found = (
                    found
                    + jnp.dot(price_high, onehot, preferred_element_type=F32)
                    + jnp.dot(price_low, onehot, preferred_element_type=F32)
                )
            res_ref[:, columns(j)] = found
            cap = cap_ref[:, columns(j)]
            weight = diag_ref[:, columns(j)] + penalty
            fixed = linear_ref[:, columns(j)]
            if first:
                fixed = fixed - penalty * 0.5 * cap

            def part(s, sums):
                gap, square = sums
                here = (scen_rows(s), columns(j))
                value = x_ref[here]
                low = low_ref[here]
                high = high_ref[here]
                rest = cap - value
                residual = res_ref[here] + weight * value + fixed - low + high
                scale = step / (weight + low / value + high / rest)
                if first:
                    res_ref[here] = residual * scale
                else:
                    res_ref[here] = residual
                    inv_ref[here] = scale
                low_ref[here] = keep * low
                high_ref[here] = keep * high
                return gap + (value * low + rest * high), square + residual * residual

            zero = jnp.zeros((periods, tile), F32)
            gap, square = lax.fori_loop(0, scens, part, (zero, zero), unroll=2)
            gap_row = gap_row + fold(gap)
            square_row = square_row + fold(square)
        return gap_row, square_row

    def exchange(k, first):
        send(
            NEAR,
            line_to,
            lambda t: ns_ref,
            lambda slot: nr_ref.at[slot],
        )
        if not first:
            send(
                PLAN,
                scen_to,
                lambda t: pg_ref.at[pl.ds(own, plan_rows)],
                lambda slot: pg_ref.at[pl.ds(own, plan_rows)],
            )
        wait_for(recv_sem.at[NEAR], spans[NEAR])
        near = ns_ref[...]
        for slot in range(depth - 1):
            near = near + nr_ref[slot]
        fs_ref[...] = near
        turn = lax.rem(k, 2)
        send(
            FAR,
            plane_to,
            lambda t: fs_ref,
            lambda slot: fr_ref.at[turn, slot],
            far_sem.at[turn],
        )
        if not first:
            wait_for(recv_sem.at[IMB], spans[IMB])
        lumped = jnp.zeros((periods, zones), F32)
        for s in range(scens):
            lumped = lumped + imb_ref[s * periods : (s + 1) * periods, :]
        both = jnp.concatenate(two_parts(lumped), axis=0)
        for j in range(blocks):
            found = jnp.dot(both, onehot_ref[:, columns(j)], preferred_element_type=F32)
            more_ref[:, columns(j)] = found[:periods] + found[periods:]
        if not first:
            wait_for(recv_sem.at[PLAN], spans[PLAN])
            for j in range(blocks):
                pieces = [
                    jnp.concatenate(
                        [
                            pg_ref[
                                pl.ds(h * 8 * plan_rows + j * tiles + t, 8, stride=plan_rows), :
                            ]
                            for t in range(tiles)
                        ],
                        axis=1,
                    )
                    for h in range(halves)
                ]
                plan = jnp.concatenate(pieces, axis=0)
                plan_ref[:, columns(j)] = plan
                twice = penalty * plan

                def settle(s, none):
                    here = (scen_rows(s), columns(j))
                    res_ref[here] = (res_ref[here] - twice) * inv_ref[here]
                    return none

                lax.fori_loop(0, scens, settle, 0, unroll=4)
        wait_for(far_sem.at[turn], spans[FAR])
        every = fs_ref[...]
        for slot in range(n_g * sides - 1):
            every = every + fr_ref[turn, slot]
        all_ref[...] = jnp.broadcast_to(jnp.sum(every, axis=1, keepdims=True), (4, LANES))

    def scalars(step):
        every = all_ref[:, 0:1]
        dual_rms = jnp.sqrt(every[0:1] / entries + epsilon)
        primal_rms = jnp.sqrt(every[1:2] / zone_entries + epsilon)
        target = centering * every[2:3] / (2.0 * entries)
        return 1.0 / (1.0 + dual_rms), step / (1.0 + primal_rms), step * target

    step = step_of(0)
    gap_row, square_row = residuals(step, True)
    wait_for(recv_sem.at[START], spans[START])
    per_zone = jnp.sum(zc_ref[...], axis=0)

    def imbalances(s, none):
        here = scen_rows(s)
        imb_ref[here, :] = level(s, (periods, zones)) * per_zone * zone_scale - load_ref[here, :]
        return none

    lax.fori_loop(0, scens, imbalances, 0, unroll=2)
    imbalance = imb_ref[mine, :]
    ns_ref[0:1, :] = square_row
    ns_ref[1:2, :] = fold(imbalance * imbalance)
    ns_ref[2:3, :] = gap_row
    exchange(0, True)
    wait_for(send_sem.at[START], spans[START])
    for kind in (NEAR, FAR):
        wait_for(send_sem.at[kind], spans[kind])

    def iteration(k, carry):
        step = step_of(k)
        shrink, pay, pull = scalars(step)

        for j in range(blocks):
            cap = cap_ref[:, columns(j)]
            lowest = 0.02 * cap
            highest = 0.98 * cap

            def update(s, sums):
                column, rounded, dual = sums
                here = (scen_rows(s), columns(j))
                value = jnp.clip(x_ref[here] - res_ref[here] * shrink, lowest, highest)
                low = low_ref[here] + pull / value
                high = high_ref[here] + pull / (cap - value)
                x_ref[here] = value
                low_ref[here] = low
                high_ref[here] = high
                return (
                    column + value,
                    rounded + value.astype(BF16).astype(F32),
                    dual + (high - low),
                )

            zero = jnp.zeros((periods, tile), F32)
            column, rounded, dual = lax.fori_loop(
                0, scens, update, (zero, zero, zero), unroll=4
            )
            column_ref[:, columns(j)] = column
            round_ref[:, columns(j)] = rounded
            dual_ref[:, columns(j)] = dual

        for j in range(blocks):
            both = jnp.concatenate(two_parts(round_ref[:, columns(j)]), axis=0)
            found = jnp.dot(both, cost_ref[j], preferred_element_type=F32) + jnp.dot(
                both, masked_ref[j], preferred_element_type=F32
            )
            paid = paid_ref[:, columns(j)] + pay * more_ref[:, columns(j)]
            paid_ref[:, columns(j)] = paid
            column = column_ref[:, columns(j)]
            rest = (
                (found[:periods] + found[periods:])
                + (diag_ref[:, columns(j)] + penalty) * column
                + float(scens) * linear_ref[:, columns(j)]
                + paid
                + dual_ref[:, columns(j)]
            )
            for t in range(tiles):
                lanes = slice(t * LANES, (t + 1) * LANES)
                for h in range(halves):
                    first = h * 8 * group + j * tiles + t
                    cs_ref[pl.ds(first, 8, stride=group), :] = column[h * 8 : h * 8 + 8, lanes]
                    cs_ref[pl.ds(first + lane_tiles, 8, stride=group), :] = rest[
                        h * 8 : h * 8 + 8, lanes
                    ]
        send(
            COLUMN,
            scen_to,
            lambda t: cs_ref.at[pl.ds(t * group, group)],
            lambda slot: cr_ref.at[pl.ds(slot * group, group)],
        )
        prices_ref[...] += pay * imb_ref[...]

        found = None
        for j in range(blocks):
            for piece in two_parts(x_ref[:, columns(j)]):
                term = jnp.dot(piece, turned_ref[columns(j), :], preferred_element_type=F32)
                found = term if found is None else found + term
        zp_ref[...] = found
        send(
            ZONE,
            gen_to,
            lambda t: zp_ref.at[pl.ds(t * share, share)],
            lambda slot: zr_ref.at[pl.ds(slot * share, share)],
        )

        gap_row, square_row = residuals(step_of(k + 1), False)

        wait_for(recv_sem.at[ZONE], spans[ZONE])
        total = zp_ref[mine, :]
        for slot in range(n_g - 1):
            total = total + zr_ref[slot * share : (slot + 1) * share, :]
        imbalance = total * zone_scale - load_ref[mine, :]
        imb_ref[mine, :] = imbalance
        send(IMB, gen_to, lambda t: imb_ref.at[mine], lambda slot: imb_ref.at[mine])
        ns_ref[1:2, :] = fold(imbalance * imbalance)
        ns_ref[2:3, :] = gap_row

        wait_for(recv_sem.at[COLUMN], spans[COLUMN])
        sums = cs_ref[pl.ds(pl.multiple_of(me_s * group, 8), group), :]
        for slot in range(n_s - 1):
            sums = sums + cr_ref[slot * group : (slot + 1) * group, :]
        plan = sums[:lane_tiles] / total_scen
        rest = sums[lane_tiles : 2 * lane_tiles]
        term = (2.0 * penalty) * plan * ((penalty / 2.0) * total_scen * plan - rest)
        ns_ref[0:1, :] = square_row + jnp.sum(term, axis=0, keepdims=True)
        pg_ref[pl.ds(own, lane_tiles), :] = plan
        exchange(k + 1, False)
        for kind in (ZONE, COLUMN, PLAN, IMB, NEAR, FAR):
            wait_for(send_sem.at[kind], spans[kind])
        return carry

    lax.fori_loop(0, ITERS - 1, iteration, 0)

    shrink, pay, _ = scalars(step_of(ITERS - 1))
    prices_ref[...] += pay * imb_ref[...]
    for j in range(blocks):
        cap = cap_ref[:, columns(j)]
        lowest = 0.02 * cap
        highest = 0.98 * cap

        def finish(s, none):
            here = (scen_rows(s), columns(j))
            x_ref[here] = jnp.clip(x_ref[here] - res_ref[here] * shrink, lowest, highest)
            return none

        lax.fori_loop(0, scens, finish, 0, unroll=4)


def solution(mesh):
    n_s, n_g = mesh.shape["scen"], mesh.shape["gen"]
    scen_dims = (n_s // 2, 2)
    gen_dims = (2, n_g // 4, 2) if n_g >= 4 else (n_g, 1, 1)

    def local(
        zone_load,
        linear_cost,
        cost_diag,
        capacity,
        cost_tiles,
        coupling_tiles,
        block_map,
        zone_index,
        step_numer,
        step_denom,
    ):
        scens, periods, zones = zone_load.shape
        width = capacity.shape[0]
        blocks, tile, _ = cost_tiles.shape
        rows = scens * periods
        lane_tiles = width // LANES
        group = -(-(2 * lane_tiles) // 8) * 8
        plan_rows = -(-lane_tiles // 8) * 8
        entries = float(n_s * rows * width * n_g)
        zone_entries = float(n_s * rows * zones)
        vmem = pl.BlockSpec(memory_space=pltpu.VMEM)
        smem = pl.BlockSpec(memory_space=pltpu.SMEM)
        state = pltpu.VMEM((rows, width), F32)
        share = rows // n_g
        dispatch, prices, plan = pl.pallas_call(
            functools.partial(
                kernel,
                scen_dims,
                gen_dims,
                entries,
                zone_entries,
                zones / (width * n_g),
            ),
            out_shape=(
                jax.ShapeDtypeStruct((rows, width), F32),
                jax.ShapeDtypeStruct((rows, zones), F32),
                jax.ShapeDtypeStruct((periods, width), F32),
            ),
            in_specs=[vmem] * 6 + [smem, vmem, smem, smem],
            out_specs=(vmem, vmem, vmem),
            scratch_shapes=[
                state,
                state,
                state,
                state,
                pltpu.VMEM((zones, width), BF16),
                pltpu.VMEM((width, zones), BF16),
                pltpu.VMEM((blocks, tile, tile), BF16),
                pltpu.VMEM((1, width), F32),
                pltpu.VMEM((1, width), F32),
                pltpu.VMEM((periods, width), F32),
                pltpu.VMEM((periods, width), F32),
                pltpu.VMEM((periods, width), F32),
                pltpu.VMEM((periods, width), F32),
                pltpu.VMEM((periods, width), F32),
                pltpu.VMEM((n_g, 1, zones), F32),
                pltpu.VMEM((rows, zones), F32),
                pltpu.VMEM(((n_g - 1) * share, zones), F32),
                pltpu.VMEM((periods * group, LANES), F32),
                pltpu.VMEM(((n_s - 1) * group, LANES), F32),
                pltpu.VMEM((n_s * plan_rows, LANES), F32),
                pltpu.VMEM((rows, zones), F32),
                pltpu.VMEM((4, LANES), F32),
                pltpu.VMEM((scen_dims[0] - 1, 4, LANES), F32),
                pltpu.VMEM((4, LANES), F32),
                pltpu.VMEM((2, n_g * scen_dims[1] - 1, 4, LANES), F32),
                pltpu.VMEM((4, LANES), F32),
                pltpu.SemaphoreType.DMA((7,)),
                pltpu.SemaphoreType.DMA((7,)),
                pltpu.SemaphoreType.DMA((2,)),
            ],
            compiler_params=pltpu.CompilerParams(collective_id=0, has_side_effects=True),
        )(
            zone_load.reshape(rows, zones),
            linear_cost,
            cost_diag,
            capacity,
            cost_tiles,
            coupling_tiles[0],
            block_map,
            zone_index,
            step_numer,
            step_denom,
        )
        return dispatch.reshape(scens, periods, width), prices.reshape(scens, periods, zones), plan

    return jax.shard_map(
        local,
        mesh=mesh,
        in_specs=(
            P("scen", None, None),
            P(None, "gen"),
            P("gen"),
            P("gen"),
            P("gen", None, None),
            P("scen", "gen", None, None),
            P("scen", "gen"),
            P("gen"),
            P(),
            P(),
        ),
        out_specs=(P("scen", None, "gen"), P("scen", None, None), P(None, "gen")),
        check_vma=False,
    )
```

```python
import functools
import itertools

import jax
import jax.numpy as jnp
from jax import lax
from jax.experimental import pallas as pl
from jax.experimental.pallas import tpu as pltpu
from jax.sharding import PartitionSpec as P

ITERS = 5
MESH = pl.DeviceIdType.MESH
F32 = jnp.float32
BF16 = jnp.bfloat16
LANES = 128

penalty = 2.0
centering = 0.5
epsilon = 1e-06


def ring(offset, size):
    return min(offset, size - offset)


def partners(dims, hops):
    result = []
    for offset in itertools.product(*[range(n) for n in dims]):
        if not any(offset):
            continue
        back = 0
        for o, n in zip(offset, dims):
            back = back * n + (n - o) % n
        result.append((hops(offset), offset, back - 1))
    result.sort(key=lambda item: -item[0])
    return [(offset, slot) for _, offset, slot in result]


def moved(me, dims, offset):
    index = 0
    stride = 1
    for n, o in zip(reversed(dims), reversed(offset)):
        coordinate = (me // stride) % n
        index = index + ((coordinate + o) % n) * stride
        stride *= n
    return index


def two_parts(value):
    high = value.astype(BF16)
    return high, (value - high.astype(F32)).astype(BF16)


def kernel(
    scen_dims,
    gen_dims,
    entries,
    zone_entries,
    zone_scale,
    load_hbm,
    linear_hbm,
    diag_hbm,
    cap_hbm,
    cost_hbm,
    coupling_hbm,
    map_hbm,
    zone_hbm,
    numer_hbm,
    denom_hbm,
    x_ref,
    prices_ref,
    plan_ref,
    load_ref,
    linear_ref,
    diag_in,
    cap_in,
    cost_ref,
    coupling_ref,
    map_ref,
    zone_in,
    numer_ref,
    denom_ref,
    low_ref,
    high_ref,
    res_ref,
    inv_ref,
    onehot_ref,
    turned_ref,
    masked_ref,
    diag_ref,
    cap_ref,
    column_ref,
    round_ref,
    dual_ref,
    paid_ref,
    more_ref,
    zc_ref,
    zp_ref,
    zr_ref,
    cs_ref,
    cr_ref,
    pg_ref,
    imb_ref,
    ns_ref,
    nr_ref,
    fs_ref,
    fr_ref,
    all_ref,
    send_sem,
    recv_sem,
    far_sem,
    in_sem,
):
    me_s = lax.axis_index("scen")
    me_g = lax.axis_index("gen")
    depth, sides = scen_dims
    n_s = depth * sides
    n_g = gen_dims[0] * gen_dims[1] * gen_dims[2]
    y_hops = {(0, 0): 0, (0, 1): 1, (1, 0): 2, (1, 1): 1}

    def scen_device(offset):
        return {"scen": moved(me_s, scen_dims, offset)}

    def gen_device(offset):
        return {"gen": moved(me_g, gen_dims, offset)}

    def plane_device(offset):
        return {
            "scen": moved(me_s, scen_dims, (0, offset[0])),
            "gen": moved(me_g, gen_dims, offset[1:]),
        }

    scen_group = partners(scen_dims, lambda o: ring(o[0], depth) + 2 * o[1])
    gen_group = partners(gen_dims, lambda o: 2 * o[0] + 2 * ring(o[1], gen_dims[1]) + o[2])
    line_group = partners((depth,), lambda o: ring(o[0], depth))
    plane_group = partners(
        (sides,) + gen_dims,
        lambda o: 2 * y_hops[o[:2]] + 2 * ring(o[2], gen_dims[1]) + o[3],
    )
    scen_to = [(scen_device(o), moved(me_s, scen_dims, o), slot) for o, slot in scen_group]
    gen_to = [(gen_device(o), moved(me_g, gen_dims, o), slot) for o, slot in gen_group]
    line_to = [(scen_device((o[0], 0)), 0, slot) for o, slot in line_group]
    plane_to = [(plane_device(o), 0, slot) for o, slot in plane_group]

    barrier = pltpu.get_barrier_semaphore()
    greeted = [device for device, _, _ in scen_to]
    greeted += [plane_device(o) for o, _ in plane_group if any(o[1:])]
    for device in greeted:
        pl.semaphore_signal(barrier, inc=1, device_id=device, device_id_type=MESH)

    fetched = {}
    for position, (name, source, place) in enumerate(
        (
            ("zone", zone_hbm, zone_in),
            ("cap", cap_hbm, cap_in),
            ("diag", diag_hbm, diag_in),
            ("cost", cost_hbm, cost_ref),
            ("map", map_hbm, map_ref),
            ("coupling", coupling_hbm, coupling_ref),
            ("linear", linear_hbm, linear_ref),
            ("numer", numer_hbm, numer_ref),
            ("denom", denom_hbm, denom_ref),
            ("load", load_hbm, load_ref),
        )
    ):
        fetched[name] = pltpu.make_async_copy(source, place, in_sem.at[position])
        fetched[name].start()

    rows, width = x_ref.shape
    periods = plan_ref.shape[0]
    scens = rows // periods
    zones = zp_ref.shape[1]
    blocks, tile, _ = cost_ref.shape
    tiles = tile // LANES
    lane_tiles = width // LANES
    halves = periods // 8
    group = cs_ref.shape[0] // periods
    share = rows // n_g
    plan_rows = pg_ref.shape[0] // n_s
    total_scen = scens * n_s
    mine = pl.ds(pl.multiple_of(me_g * share, share), share)
    own = pl.multiple_of(me_s * plan_rows, plan_rows)

    def columns(j):
        return pl.ds(j * tile, tile)

    def scen_rows(s):
        return pl.ds(pl.multiple_of(s * periods, periods), periods)

    def send(kind, to, source, landing, sem=None):
        for device, member, slot in to:
            pltpu.make_async_remote_copy(
                src_ref=source(member),
                dst_ref=landing(slot),
                send_sem=send_sem.at[kind],
                recv_sem=recv_sem.at[kind] if sem is None else sem,
                device_id=device,
                device_id_type=MESH,
            ).start()

    def wait_for(sem, span):
        pltpu.make_async_copy(span, span, sem).wait()

    ZONE, COLUMN, PLAN, IMB, NEAR, FAR, START = range(7)
    spans = {
        ZONE: zr_ref,
        COLUMN: cr_ref,
        PLAN: pg_ref.at[pl.ds(0, (n_s - 1) * plan_rows)],
        IMB: imb_ref.at[pl.ds(0, (n_g - 1) * share)],
        NEAR: nr_ref,
        FAR: fr_ref.at[0],
        START: zc_ref.at[pl.ds(0, n_g - 1)],
    }

    def level(s, shape):
        ids = jnp.full(shape, me_s * scens + s, jnp.int32)
        return 0.2 + 0.6 * (ids.astype(F32) + 0.5) / total_scen

    def step_of(k):
        numer = jnp.full((1, 1), numer_ref[k], jnp.int32).astype(F32)
        return numer / jnp.full((1, 1), denom_ref[k], jnp.int32).astype(F32)

    def fold(value):
        row = jnp.sum(value, axis=0, keepdims=True)
        return sum(row[:, t * LANES : (t + 1) * LANES] for t in range(value.shape[1] // LANES))

    for name in ("zone", "cap", "diag"):
        fetched[name].wait()
    diag_ref[...] = diag_in[...].reshape(1, width)
    cap_ref[...] = cap_in[...].reshape(1, width)
    zone_row = zone_in[...].reshape(1, width)
    start = jnp.zeros((16, zones), F32)
    for j in range(blocks):
        ids = lax.broadcasted_iota(jnp.int32, (zones, tile), 0)
        onehot = jnp.where(ids == zone_row[:, j * tile : (j + 1) * tile], 1.0, 0.0)
        onehot_ref[:, columns(j)] = onehot.astype(BF16)
        turned = onehot.T.astype(BF16)
        turned_ref[columns(j), :] = turned
        cap_high, cap_low = two_parts(jnp.broadcast_to(cap_ref[:, columns(j)], (8, tile)))
        both = jnp.concatenate([cap_high, cap_low], axis=0)
        start = start + jnp.dot(both, turned, preferred_element_type=F32)
    zc_ref[me_g] = start[0:1] + start[8:9]

    pl.semaphore_wait(barrier, len(greeted))
    send(START, gen_to, lambda t: zc_ref.at[me_g], lambda slot: zc_ref.at[me_g])

    for name in ("map", "coupling"):
        fetched[name].wait()
    for j in range(blocks):
        mask = map_ref[0, j].astype(F32)
        masked_ref[j] = (coupling_ref[j].astype(F32) * mask).astype(BF16)

    def begin(s, carry):
        here = scen_rows(s)
        x_ref[here, :] = level(s, (periods, width)) * cap_ref[...]
        low_ref[here, :] = jnp.ones((periods, width), F32)
        high_ref[here, :] = jnp.ones((periods, width), F32)
        return carry

    lax.fori_loop(0, scens, begin, 0, unroll=2)
    prices_ref[...] = jnp.zeros_like(prices_ref)
    paid_ref[...] = jnp.zeros_like(paid_ref)
    cs_ref[...] = jnp.zeros_like(cs_ref)
    ns_ref[...] = jnp.zeros_like(ns_ref)
    pg_ref[...] = jnp.zeros_like(pg_ref)

    def residuals(step, first):
        if not first:
            price_high, price_low = two_parts(prices_ref[...])
        gap_row = jnp.zeros((1, LANES), F32)
        square_row = jnp.zeros((1, LANES), F32)
        keep = 1.0 - step
        for j in range(blocks):
            left = x_ref[:, columns(j)].astype(BF16)
            found = jnp.dot(left, cost_ref[j], preferred_element_type=F32) + jnp.dot(
                left, masked_ref[j], preferred_element_type=F32
            )
            if not first:
                onehot = onehot_ref[:, columns(j)]
                found = (
                    found
                    + jnp.dot(price_high, onehot, preferred_element_type=F32)
                    + jnp.dot(price_low, onehot, preferred_element_type=F32)
                )
            res_ref[:, columns(j)] = found
            cap = cap_ref[:, columns(j)]
            weight = diag_ref[:, columns(j)] + penalty
            fixed = linear_ref[:, columns(j)]
            if first:
                fixed = fixed - penalty * 0.5 * cap

            def part(s, sums):
                gap, square = sums
                here = (scen_rows(s), columns(j))
                value = x_ref[here]
                low = low_ref[here]
                high = high_ref[here]
                rest = cap - value
                residual = res_ref[here] + weight * value + fixed - low + high
                scale = step / (weight + low / value + high / rest)
                if first:
                    res_ref[here] = residual * scale
                else:
                    res_ref[here] = residual
                    inv_ref[here] = scale
                low_ref[here] = keep * low
                high_ref[here] = keep * high
                return gap + (value * low + rest * high), square + residual * residual

            zero = jnp.zeros((periods, tile), F32)
            gap, square = lax.fori_loop(0, scens, part, (zero, zero), unroll=2)
            gap_row = gap_row + fold(gap)
            square_row = square_row + fold(square)
        return gap_row, square_row

    def exchange(k, first):
        send(
            NEAR,
            line_to,
            lambda t: ns_ref,
            lambda slot: nr_ref.at[slot],
        )
        if not first:
            send(
                PLAN,
                scen_to,
                lambda t: pg_ref.at[pl.ds(own, plan_rows)],
                lambda slot: pg_ref.at[pl.ds(own, plan_rows)],
            )
        wait_for(recv_sem.at[NEAR], spans[NEAR])
        near = ns_ref[...]
        for slot in range(depth - 1):
            near = near + nr_ref[slot]
        fs_ref[...] = near
        turn = lax.rem(k, 2)
        send(
            FAR,
            plane_to,
            lambda t: fs_ref,
            lambda slot: fr_ref.at[turn, slot],
            far_sem.at[turn],
        )
        if not first:
            wait_for(recv_sem.at[IMB], spans[IMB])
        lumped = jnp.zeros((periods, zones), F32)
        for s in range(scens):
            lumped = lumped + imb_ref[s * periods : (s + 1) * periods, :]
        both = jnp.concatenate(two_parts(lumped), axis=0)
        for j in range(blocks):
            found = jnp.dot(both, onehot_ref[:, columns(j)], preferred_element_type=F32)
            more_ref[:, columns(j)] = found[:periods] + found[periods:]
        if not first:
            wait_for(recv_sem.at[PLAN], spans[PLAN])
            for j in range(blocks):
                pieces = [
                    jnp.concatenate(
                        [
                            pg_ref[
                                pl.ds(h * 8 * plan_rows + j * tiles + t, 8, stride=plan_rows), :
                            ]
                            for t in range(tiles)
                        ],
                        axis=1,
                    )
                    for h in range(halves)
                ]
                plan = jnp.concatenate(pieces, axis=0)
                plan_ref[:, columns(j)] = plan
                twice = penalty * plan

                def settle(s, none):
                    here = (scen_rows(s), columns(j))
                    res_ref[here] = (res_ref[here] - twice) * inv_ref[here]
                    return none

                lax.fori_loop(0, scens, settle, 0, unroll=4)
        wait_for(far_sem.at[turn], spans[FAR])
        every = fs_ref[...]
        for slot in range(n_g * sides - 1):
            every = every + fr_ref[turn, slot]
        all_ref[...] = jnp.broadcast_to(jnp.sum(every, axis=1, keepdims=True), (4, LANES))

    def scalars(step):
        every = all_ref[:, 0:1]
        dual_rms = jnp.sqrt(every[0:1] / entries + epsilon)
        primal_rms = jnp.sqrt(every[1:2] / zone_entries + epsilon)
        target = centering * every[2:3] / (2.0 * entries)
        return 1.0 / (1.0 + dual_rms), step / (1.0 + primal_rms), step * target

    for name in ("numer", "denom", "linear", "cost"):
        fetched[name].wait()
    step = step_of(0)
    gap_row, square_row = residuals(step, True)
    fetched["load"].wait()
    wait_for(recv_sem.at[START], spans[START])
    per_zone = jnp.sum(zc_ref[...], axis=0)

    def imbalances(s, none):
        here = scen_rows(s)
        imb_ref[here, :] = level(s, (periods, zones)) * per_zone * zone_scale - load_ref[here, :]
        return none

    lax.fori_loop(0, scens, imbalances, 0, unroll=2)
    imbalance = imb_ref[mine, :]
    ns_ref[0:1, :] = square_row
    ns_ref[1:2, :] = fold(imbalance * imbalance)
    ns_ref[2:3, :] = gap_row
    exchange(0, True)
    wait_for(send_sem.at[START], spans[START])
    for kind in (NEAR, FAR):
        wait_for(send_sem.at[kind], spans[kind])

    def iteration(k, carry):
        step = step_of(k)
        shrink, pay, pull = scalars(step)

        for j in range(blocks):
            cap = cap_ref[:, columns(j)]
            lowest = 0.02 * cap
            highest = 0.98 * cap

            def update(s, sums):
                column, rounded, dual = sums
                here = (scen_rows(s), columns(j))
                value = jnp.clip(x_ref[here] - res_ref[here] * shrink, lowest, highest)
                low = low_ref[here] + pull / value
                high = high_ref[here] + pull / (cap - value)
                x_ref[here] = value
                low_ref[here] = low
                high_ref[here] = high
                return (
                    column + value,
                    rounded + value.astype(BF16).astype(F32),
                    dual + (high - low),
                )

            zero = jnp.zeros((periods, tile), F32)
            column, rounded, dual = lax.fori_loop(
                0, scens, update, (zero, zero, zero), unroll=4
            )
            column_ref[:, columns(j)] = column
            round_ref[:, columns(j)] = rounded
            dual_ref[:, columns(j)] = dual

        for j in range(blocks):
            both = jnp.concatenate(two_parts(round_ref[:, columns(j)]), axis=0)
            found = jnp.dot(both, cost_ref[j], preferred_element_type=F32) + jnp.dot(
                both, masked_ref[j], preferred_element_type=F32
            )
            paid = paid_ref[:, columns(j)] + pay * more_ref[:, columns(j)]
            paid_ref[:, columns(j)] = paid
            column = column_ref[:, columns(j)]
            rest = (
                (found[:periods] + found[periods:])
                + (diag_ref[:, columns(j)] + penalty) * column
                + float(scens) * linear_ref[:, columns(j)]
                + paid
                + dual_ref[:, columns(j)]
            )
            for t in range(tiles):
                lanes = slice(t * LANES, (t + 1) * LANES)
                for h in range(halves):
                    first = h * 8 * group + j * tiles + t
                    cs_ref[pl.ds(first, 8, stride=group), :] = column[h * 8 : h * 8 + 8, lanes]
                    cs_ref[pl.ds(first + lane_tiles, 8, stride=group), :] = rest[
                        h * 8 : h * 8 + 8, lanes
                    ]
        send(
            COLUMN,
            scen_to,
            lambda t: cs_ref.at[pl.ds(t * group, group)],
            lambda slot: cr_ref.at[pl.ds(slot * group, group)],
        )
        prices_ref[...] += pay * imb_ref[...]

        found = None
        for j in range(blocks):
            for piece in two_parts(x_ref[:, columns(j)]):
                term = jnp.dot(piece, turned_ref[columns(j), :], preferred_element_type=F32)
                found = term if found is None else found + term
        zp_ref[...] = found
        send(
            ZONE,
            gen_to,
            lambda t: zp_ref.at[pl.ds(t * share, share)],
            lambda slot: zr_ref.at[pl.ds(slot * share, share)],
        )

        gap_row, square_row = residuals(step_of(k + 1), False)

        wait_for(recv_sem.at[ZONE], spans[ZONE])
        total = zp_ref[mine, :]
        for slot in range(n_g - 1):
            total = total + zr_ref[slot * share : (slot + 1) * share, :]
        imbalance = total * zone_scale - load_ref[mine, :]
        imb_ref[mine, :] = imbalance
        send(IMB, gen_to, lambda t: imb_ref.at[mine], lambda slot: imb_ref.at[mine])
        ns_ref[1:2, :] = fold(imbalance * imbalance)
        ns_ref[2:3, :] = gap_row

        wait_for(recv_sem.at[COLUMN], spans[COLUMN])
        sums = cs_ref[pl.ds(pl.multiple_of(me_s * group, 8), group), :]
        for slot in range(n_s - 1):
            sums = sums + cr_ref[slot * group : (slot + 1) * group, :]
        plan = sums[:lane_tiles] / total_scen
        rest = sums[lane_tiles : 2 * lane_tiles]
        term = (2.0 * penalty) * plan * ((penalty / 2.0) * total_scen * plan - rest)
        ns_ref[0:1, :] = square_row + jnp.sum(term, axis=0, keepdims=True)
        pg_ref[pl.ds(own, lane_tiles), :] = plan
        exchange(k + 1, False)
        for kind in (ZONE, COLUMN, PLAN, IMB, NEAR, FAR):
            wait_for(send_sem.at[kind], spans[kind])
        return carry

    lax.fori_loop(0, ITERS - 1, iteration, 0)

    shrink, pay, _ = scalars(step_of(ITERS - 1))
    prices_ref[...] += pay * imb_ref[...]
    for j in range(blocks):
        cap = cap_ref[:, columns(j)]
        lowest = 0.02 * cap
        highest = 0.98 * cap

        def finish(s, none):
            here = (scen_rows(s), columns(j))
            x_ref[here] = jnp.clip(x_ref[here] - res_ref[here] * shrink, lowest, highest)
            return none

        lax.fori_loop(0, scens, finish, 0, unroll=4)


def solution(mesh):
    n_s, n_g = mesh.shape["scen"], mesh.shape["gen"]
    scen_dims = (n_s // 2, 2)
    gen_dims = (2, n_g // 4, 2) if n_g >= 4 else (n_g, 1, 1)

    def local(
        zone_load,
        linear_cost,
        cost_diag,
        capacity,
        cost_tiles,
        coupling_tiles,
        block_map,
        zone_index,
        step_numer,
        step_denom,
    ):
        scens, periods, zones = zone_load.shape
        width = capacity.shape[0]
        blocks, tile, _ = cost_tiles.shape
        rows = scens * periods
        lane_tiles = width // LANES
        group = -(-(2 * lane_tiles) // 8) * 8
        plan_rows = -(-lane_tiles // 8) * 8
        entries = float(n_s * rows * width * n_g)
        zone_entries = float(n_s * rows * zones)
        vmem = pl.BlockSpec(memory_space=pltpu.VMEM)
        hbm = pl.BlockSpec(memory_space=pltpu.HBM)
        state = pltpu.VMEM((rows, width), F32)
        share = rows // n_g
        dispatch, prices, plan = pl.pallas_call(
            functools.partial(
                kernel,
                scen_dims,
                gen_dims,
                entries,
                zone_entries,
                zones / (width * n_g),
            ),
            out_shape=(
                jax.ShapeDtypeStruct((rows, width), F32),
                jax.ShapeDtypeStruct((rows, zones), F32),
                jax.ShapeDtypeStruct((periods, width), F32),
            ),
            in_specs=[hbm] * 10,
            out_specs=(vmem, vmem, vmem),
            scratch_shapes=[
                pltpu.VMEM((rows, zones), F32),
                pltpu.VMEM((periods, width), F32),
                pltpu.VMEM((width,), F32),
                pltpu.VMEM((width,), F32),
                pltpu.VMEM((blocks, tile, tile), BF16),
                pltpu.VMEM((blocks, tile, tile), BF16),
                pltpu.SMEM(block_map.shape, jnp.int32),
                pltpu.VMEM((width,), jnp.int32),
                pltpu.SMEM(step_numer.shape, jnp.int32),
                pltpu.SMEM(step_denom.shape, jnp.int32),
                state,
                state,
                state,
                state,
                pltpu.VMEM((zones, width), BF16),
                pltpu.VMEM((width, zones), BF16),
                pltpu.VMEM((blocks, tile, tile), BF16),
                pltpu.VMEM((1, width), F32),
                pltpu.VMEM((1, width), F32),
                pltpu.VMEM((periods, width), F32),
                pltpu.VMEM((periods, width), F32),
                pltpu.VMEM((periods, width), F32),
                pltpu.VMEM((periods, width), F32),
                pltpu.VMEM((periods, width), F32),
                pltpu.VMEM((n_g, 1, zones), F32),
                pltpu.VMEM((rows, zones), F32),
                pltpu.VMEM(((n_g - 1) * share, zones), F32),
                pltpu.VMEM((periods * group, LANES), F32),
                pltpu.VMEM(((n_s - 1) * group, LANES), F32),
                pltpu.VMEM((n_s * plan_rows, LANES), F32),
                pltpu.VMEM((rows, zones), F32),
                pltpu.VMEM((4, LANES), F32),
                pltpu.VMEM((scen_dims[0] - 1, 4, LANES), F32),
                pltpu.VMEM((4, LANES), F32),
                pltpu.VMEM((2, n_g * scen_dims[1] - 1, 4, LANES), F32),
                pltpu.VMEM((4, LANES), F32),
                pltpu.SemaphoreType.DMA((7,)),
                pltpu.SemaphoreType.DMA((7,)),
                pltpu.SemaphoreType.DMA((2,)),
                pltpu.SemaphoreType.DMA((10,)),
            ],
            compiler_params=pltpu.CompilerParams(collective_id=0, has_side_effects=True),
        )(
            zone_load.reshape(rows, zones),
            linear_cost,
            cost_diag,
            capacity,
            cost_tiles,
            coupling_tiles[0],
            block_map,
            zone_index,
            step_numer,
            step_denom,
        )
        return dispatch.reshape(scens, periods, width), prices.reshape(scens, periods, zones), plan

    return jax.shard_map(
        local,
        mesh=mesh,
        in_specs=(
            P("scen", None, None),
            P(None, "gen"),
            P("gen"),
            P("gen"),
            P("gen", None, None),
            P("scen", "gen", None, None),
            P("scen", "gen"),
            P("gen"),
            P(),
            P(),
        ),
        out_specs=(P("scen", None, "gen"), P("scen", None, None), P(None, "gen")),
        check_vma=False,
    )
```

```python
import functools
import itertools

import jax
import jax.numpy as jnp
from jax import lax
from jax.experimental import pallas as pl
from jax.experimental.pallas import tpu as pltpu
from jax.sharding import PartitionSpec as P

ITERS = 5
MESH = pl.DeviceIdType.MESH
F32 = jnp.float32
BF16 = jnp.bfloat16
LANES = 128

penalty = 2.0
centering = 0.5
epsilon = 1e-06


def ring(offset, size):
    return min(offset, size - offset)


def partners(dims, hops):
    result = []
    for offset in itertools.product(*[range(n) for n in dims]):
        if not any(offset):
            continue
        back = 0
        for o, n in zip(offset, dims):
            back = back * n + (n - o) % n
        result.append((hops(offset), offset, back - 1))
    result.sort(key=lambda item: -item[0])
    return [(offset, slot) for _, offset, slot in result]


def moved(me, dims, offset):
    index = 0
    stride = 1
    for n, o in zip(reversed(dims), reversed(offset)):
        coordinate = (me // stride) % n
        index = index + ((coordinate + o) % n) * stride
        stride *= n
    return index


def two_parts(value):
    high = value.astype(BF16)
    return high, (value - high.astype(F32)).astype(BF16)


def kernel(
    scen_dims,
    gen_dims,
    entries,
    zone_entries,
    zone_scale,
    load_hbm,
    linear_hbm,
    diag_hbm,
    cap_hbm,
    cost_hbm,
    coupling_hbm,
    map_hbm,
    zone_hbm,
    numer_hbm,
    denom_hbm,
    x_out,
    prices_out,
    plan_out,
    x_ref,
    prices_ref,
    plan_ref,
    load_ref,
    linear_ref,
    diag_in,
    cap_in,
    cost_ref,
    coupling_ref,
    map_ref,
    zone_in,
    numer_ref,
    denom_ref,
    low_ref,
    high_ref,
    res_ref,
    inv_ref,
    onehot_ref,
    turned_ref,
    masked_ref,
    diag_ref,
    cap_ref,
    column_ref,
    round_ref,
    dual_ref,
    paid_ref,
    more_ref,
    zc_ref,
    zp_ref,
    zr_ref,
    cs_ref,
    cr_ref,
    pg_ref,
    imb_ref,
    ns_ref,
    nr_ref,
    fs_ref,
    fr_ref,
    wide_ref,
    all_ref,
    send_sem,
    recv_sem,
    far_sem,
    in_sem,
    out_sem,
):
    me_s = lax.axis_index("scen")
    me_g = lax.axis_index("gen")
    depth, sides = scen_dims
    n_s = depth * sides
    n_g = gen_dims[0] * gen_dims[1] * gen_dims[2]
    y_hops = {(0, 0): 0, (0, 1): 1, (1, 0): 2, (1, 1): 1}

    def scen_device(offset):
        return {"scen": moved(me_s, scen_dims, offset)}

    def gen_device(offset):
        return {"gen": moved(me_g, gen_dims, offset)}

    def plane_device(offset):
        return {
            "scen": moved(me_s, scen_dims, (0, offset[0])),
            "gen": moved(me_g, gen_dims, offset[1:]),
        }

    scen_group = partners(scen_dims, lambda o: ring(o[0], depth) + 2 * o[1])
    gen_group = partners(gen_dims, lambda o: 2 * o[0] + 2 * ring(o[1], gen_dims[1]) + o[2])
    line_group = partners((depth,), lambda o: ring(o[0], depth))
    plane_group = partners(
        (sides,) + gen_dims,
        lambda o: 2 * y_hops[o[:2]] + 2 * ring(o[2], gen_dims[1]) + o[3],
    )
    scen_to = [(scen_device(o), moved(me_s, scen_dims, o), slot) for o, slot in scen_group]
    gen_to = [(gen_device(o), moved(me_g, gen_dims, o), slot) for o, slot in gen_group]
    line_to = [(scen_device((o[0], 0)), 0, slot) for o, slot in line_group]
    plane_to = [(plane_device(o), 0, slot) for o, slot in plane_group]

    barrier = pltpu.get_barrier_semaphore()
    greeted = [device for device, _, _ in scen_to]
    greeted += [plane_device(o) for o, _ in plane_group if any(o[1:])]
    for device in greeted:
        pl.semaphore_signal(barrier, inc=1, device_id=device, device_id_type=MESH)

    fetched = {}
    for position, (name, source, place) in enumerate(
        (
            ("zone", zone_hbm, zone_in),
            ("cap", cap_hbm, cap_in),
            ("diag", diag_hbm, diag_in),
            ("cost", cost_hbm, cost_ref),
            ("map", map_hbm, map_ref),
            ("coupling", coupling_hbm, coupling_ref),
            ("linear", linear_hbm, linear_ref),
            ("numer", numer_hbm, numer_ref),
            ("denom", denom_hbm, denom_ref),
            ("load", load_hbm, load_ref),
        )
    ):
        fetched[name] = pltpu.make_async_copy(source, place, in_sem.at[position])
        fetched[name].start()

    rows, width = x_ref.shape
    periods = plan_ref.shape[0]
    scens = rows // periods
    zones = zp_ref.shape[1]
    blocks, tile, _ = cost_ref.shape
    tiles = tile // LANES
    lane_tiles = width // LANES
    halves = periods // 8
    group = cs_ref.shape[0] // periods
    share = rows // n_g
    plan_rows = pg_ref.shape[0] // n_s
    total_scen = scens * n_s
    mine = pl.ds(pl.multiple_of(me_g * share, share), share)
    own = pl.multiple_of(me_s * plan_rows, plan_rows)

    def columns(j):
        return pl.ds(j * tile, tile)

    def scen_rows(s):
        return pl.ds(pl.multiple_of(s * periods, periods), periods)

    def send(kind, to, source, landing, sem=None):
        for device, member, slot in to:
            pltpu.make_async_remote_copy(
                src_ref=source(member),
                dst_ref=landing(slot),
                send_sem=send_sem.at[kind],
                recv_sem=recv_sem.at[kind] if sem is None else sem,
                device_id=device,
                device_id_type=MESH,
            ).start()

    def wait_for(sem, span):
        pltpu.make_async_copy(span, span, sem).wait()

    ZONE, COLUMN, PLAN, IMB, NEAR, FAR, START, WIDE = range(8)
    spans = {
        ZONE: zr_ref,
        COLUMN: cr_ref,
        PLAN: pg_ref.at[pl.ds(0, (n_s - 1) * plan_rows)],
        IMB: imb_ref.at[pl.ds(0, (n_g - 1) * share)],
        NEAR: nr_ref,
        FAR: fr_ref.at[0],
        START: zc_ref.at[pl.ds(0, n_g - 1)],
        WIDE: wide_ref,
    }

    def level(s, shape):
        ids = jnp.full(shape, me_s * scens + s, jnp.int32)
        return 0.2 + 0.6 * (ids.astype(F32) + 0.5) / total_scen

    def step_of(k):
        numer = jnp.full((1, 1), numer_ref[k], jnp.int32).astype(F32)
        return numer / jnp.full((1, 1), denom_ref[k], jnp.int32).astype(F32)

    def fold(value):
        row = jnp.sum(value, axis=0, keepdims=True)
        return sum(row[:, t * LANES : (t + 1) * LANES] for t in range(value.shape[1] // LANES))

    for name in ("zone", "cap", "diag"):
        fetched[name].wait()
    diag_ref[...] = diag_in[...].reshape(1, width)
    cap_ref[...] = cap_in[...].reshape(1, width)
    zone_row = zone_in[...].reshape(1, width)
    start = jnp.zeros((16, zones), F32)
    for j in range(blocks):
        ids = lax.broadcasted_iota(jnp.int32, (zones, tile), 0)
        onehot = jnp.where(ids == zone_row[:, j * tile : (j + 1) * tile], 1.0, 0.0)
        onehot_ref[:, columns(j)] = onehot.astype(BF16)
        turned = onehot.T.astype(BF16)
        turned_ref[columns(j), :] = turned
        cap_high, cap_low = two_parts(jnp.broadcast_to(cap_ref[:, columns(j)], (8, tile)))
        both = jnp.concatenate([cap_high, cap_low], axis=0)
        start = start + jnp.dot(both, turned, preferred_element_type=F32)
    zc_ref[me_g] = start[0:1] + start[8:9]

    pl.semaphore_wait(barrier, len(greeted))
    send(START, gen_to, lambda t: zc_ref.at[me_g], lambda slot: zc_ref.at[me_g])

    for name in ("map", "coupling"):
        fetched[name].wait()
    for j in range(blocks):
        mask = map_ref[0, j].astype(F32)
        masked_ref[j] = (coupling_ref[j].astype(F32) * mask).astype(BF16)

    def begin(s, carry):
        here = scen_rows(s)
        x_ref[here, :] = level(s, (periods, width)) * cap_ref[...]
        low_ref[here, :] = jnp.ones((periods, width), F32)
        high_ref[here, :] = jnp.ones((periods, width), F32)
        return carry

    lax.fori_loop(0, scens, begin, 0, unroll=2)
    prices_ref[...] = jnp.zeros_like(prices_ref)
    paid_ref[...] = jnp.zeros_like(paid_ref)
    cs_ref[...] = jnp.zeros_like(cs_ref)
    ns_ref[...] = jnp.zeros_like(ns_ref)
    fs_ref[...] = jnp.zeros_like(fs_ref)
    pg_ref[...] = jnp.zeros_like(pg_ref)

    def residuals(step, first):
        if not first:
            price_high, price_low = two_parts(prices_ref[...])
        gap_row = jnp.zeros((1, LANES), F32)
        square_row = jnp.zeros((1, LANES), F32)
        keep = 1.0 - step
        for j in range(blocks):
            left = x_ref[:, columns(j)].astype(BF16)
            found = jnp.dot(left, cost_ref[j], preferred_element_type=F32) + jnp.dot(
                left, masked_ref[j], preferred_element_type=F32
            )
            if not first:
                onehot = onehot_ref[:, columns(j)]
                found = (
                    found
                    + jnp.dot(price_high, onehot, preferred_element_type=F32)
                    + jnp.dot(price_low, onehot, preferred_element_type=F32)
                )
            res_ref[:, columns(j)] = found
            cap = cap_ref[:, columns(j)]
            weight = diag_ref[:, columns(j)] + penalty
            fixed = linear_ref[:, columns(j)]
            if first:
                fixed = fixed - penalty * 0.5 * cap

            def part(s, sums):
                gap, square = sums
                here = (scen_rows(s), columns(j))
                value = x_ref[here]
                low = low_ref[here]
                high = high_ref[here]
                rest = cap - value
                residual = res_ref[here] + weight * value + fixed - low + high
                scale = step / (weight + low / value + high / rest)
                if first:
                    res_ref[here] = residual * scale
                else:
                    res_ref[here] = residual
                    inv_ref[here] = scale
                low_ref[here] = keep * low
                high_ref[here] = keep * high
                return gap + (value * low + rest * high), square + residual * residual

            zero = jnp.zeros((periods, tile), F32)
            gap, square = lax.fori_loop(0, scens, part, (zero, zero), unroll=2)
            gap_row = gap_row + fold(gap)
            square_row = square_row + fold(square)
        return gap_row, square_row

    def lump():
        lumped = jnp.zeros((periods, zones), F32)
        for s in range(scens):
            lumped = lumped + imb_ref[s * periods : (s + 1) * periods, :]
        both = jnp.concatenate(two_parts(lumped), axis=0)
        for j in range(blocks):
            found = jnp.dot(both, onehot_ref[:, columns(j)], preferred_element_type=F32)
            more_ref[:, columns(j)] = found[:periods] + found[periods:]

    def keep_sums(every):
        all_ref[...] = jnp.broadcast_to(jnp.sum(every, axis=1, keepdims=True), (4, LANES))

    def exchange(k):
        send(NEAR, line_to, lambda t: ns_ref, lambda slot: nr_ref.at[slot])
        send(
            PLAN,
            scen_to,
            lambda t: pg_ref.at[pl.ds(own, plan_rows)],
            lambda slot: pg_ref.at[pl.ds(own, plan_rows)],
        )
        wait_for(recv_sem.at[NEAR], spans[NEAR])
        near = ns_ref[...]
        for slot in range(depth - 1):
            near = near + nr_ref[slot]
        fs_ref[...] = near
        turn = lax.rem(k, 2)
        send(
            FAR,
            plane_to,
            lambda t: fs_ref,
            lambda slot: fr_ref.at[turn, slot],
            far_sem.at[turn],
        )
        wait_for(recv_sem.at[IMB], spans[IMB])
        lump()
        wait_for(recv_sem.at[PLAN], spans[PLAN])
        for j in range(blocks):
            pieces = [
                jnp.concatenate(
                    [
                        pg_ref[
                            pl.ds(h * 8 * plan_rows + j * tiles + t, 8, stride=plan_rows), :
                        ]
                        for t in range(tiles)
                    ],
                    axis=1,
                )
                for h in range(halves)
            ]
            plan = jnp.concatenate(pieces, axis=0)
            plan_ref[:, columns(j)] = plan
            twice = penalty * plan

            def settle(s, none):
                here = (scen_rows(s), columns(j))
                res_ref[here] = (res_ref[here] - twice) * inv_ref[here]
                return none

            lax.fori_loop(0, scens, settle, 0, unroll=4)
        wait_for(far_sem.at[turn], spans[FAR])
        every = fs_ref[...]
        for slot in range(n_g * sides - 1):
            every = every + fr_ref[turn, slot]
        keep_sums(every)

    def scalars(step):
        every = all_ref[:, 0:1]
        dual_rms = jnp.sqrt(every[0:1] / entries + epsilon)
        primal_rms = jnp.sqrt(every[1:2] / zone_entries + epsilon)
        target = centering * every[2:3] / (2.0 * entries)
        return 1.0 / (1.0 + dual_rms), step / (1.0 + primal_rms), step * target

    for name in ("numer", "denom", "linear", "cost"):
        fetched[name].wait()
    step = step_of(0)
    gap_row, square_row = residuals(step, True)
    fs_ref[0:1, :] = square_row
    fs_ref[2:3, :] = gap_row
    send(FAR, plane_to, lambda t: fs_ref, lambda slot: fr_ref.at[0, slot], far_sem.at[0])
    fetched["load"].wait()
    wait_for(recv_sem.at[START], spans[START])
    per_zone = jnp.sum(zc_ref[...], axis=0)

    def imbalances(s, square):
        here = scen_rows(s)
        value = level(s, (periods, zones)) * per_zone * zone_scale - load_ref[here, :]
        imb_ref[here, :] = value
        return square + value * value

    square = lax.fori_loop(0, scens, imbalances, jnp.zeros((periods, zones), F32), unroll=2)
    primal_row = fold(square)
    lump()
    wait_for(far_sem.at[0], spans[FAR])
    every = fs_ref[...]
    for slot in range(n_g * sides - 1):
        every = every + fr_ref[0, slot]
    ns_ref[...] = every * (1.0 / sides)
    ns_ref[1:2, :] = primal_row
    send(WIDE, scen_to, lambda t: ns_ref, lambda slot: wide_ref.at[slot])
    wait_for(recv_sem.at[WIDE], spans[WIDE])
    every = ns_ref[...]
    for slot in range(n_s - 1):
        every = every + wide_ref[slot]
    keep_sums(every)
    for kind in (START, FAR, WIDE):
        wait_for(send_sem.at[kind], spans[kind])

    def iteration(k, carry):
        step = step_of(k)
        shrink, pay, pull = scalars(step)

        for j in range(blocks):
            cap = cap_ref[:, columns(j)]
            lowest = 0.02 * cap
            highest = 0.98 * cap

            def update(s, sums):
                column, rounded, dual = sums
                here = (scen_rows(s), columns(j))
                value = jnp.clip(x_ref[here] - res_ref[here] * shrink, lowest, highest)
                low = low_ref[here] + pull / value
                high = high_ref[here] + pull / (cap - value)
                x_ref[here] = value
                low_ref[here] = low
                high_ref[here] = high
                return (
                    column + value,
                    rounded + value.astype(BF16).astype(F32),
                    dual + (high - low),
                )

            zero = jnp.zeros((periods, tile), F32)
            column, rounded, dual = lax.fori_loop(
                0, scens, update, (zero, zero, zero), unroll=4
            )
            column_ref[:, columns(j)] = column
            round_ref[:, columns(j)] = rounded
            dual_ref[:, columns(j)] = dual

        for j in range(blocks):
            both = jnp.concatenate(two_parts(round_ref[:, columns(j)]), axis=0)
            found = jnp.dot(both, cost_ref[j], preferred_element_type=F32) + jnp.dot(
                both, masked_ref[j], preferred_element_type=F32
            )
            paid = paid_ref[:, columns(j)] + pay * more_ref[:, columns(j)]
            paid_ref[:, columns(j)] = paid
            column = column_ref[:, columns(j)]
            rest = (
                (found[:periods] + found[periods:])
                + (diag_ref[:, columns(j)] + penalty) * column
                + float(scens) * linear_ref[:, columns(j)]
                + paid
                + dual_ref[:, columns(j)]
            )
            for t in range(tiles):
                lanes = slice(t * LANES, (t + 1) * LANES)
                for h in range(halves):
                    first = h * 8 * group + j * tiles + t
                    cs_ref[pl.ds(first, 8, stride=group), :] = column[h * 8 : h * 8 + 8, lanes]
                    cs_ref[pl.ds(first + lane_tiles, 8, stride=group), :] = rest[
                        h * 8 : h * 8 + 8, lanes
                    ]
        send(
            COLUMN,
            scen_to,
            lambda t: cs_ref.at[pl.ds(t * group, group)],
            lambda slot: cr_ref.at[pl.ds(slot * group, group)],
        )
        prices_ref[...] += pay * imb_ref[...]

        found = None
        for j in range(blocks):
            for piece in two_parts(x_ref[:, columns(j)]):
                term = jnp.dot(piece, turned_ref[columns(j), :], preferred_element_type=F32)
                found = term if found is None else found + term
        zp_ref[...] = found
        send(
            ZONE,
            gen_to,
            lambda t: zp_ref.at[pl.ds(t * share, share)],
            lambda slot: zr_ref.at[pl.ds(slot * share, share)],
        )

        gap_row, square_row = residuals(step_of(k + 1), False)

        wait_for(recv_sem.at[ZONE], spans[ZONE])
        total = zp_ref[mine, :]
        for slot in range(n_g - 1):
            total = total + zr_ref[slot * share : (slot + 1) * share, :]
        imbalance = total * zone_scale - load_ref[mine, :]
        imb_ref[mine, :] = imbalance
        send(IMB, gen_to, lambda t: imb_ref.at[mine], lambda slot: imb_ref.at[mine])
        ns_ref[1:2, :] = fold(imbalance * imbalance)
        ns_ref[2:3, :] = gap_row

        wait_for(recv_sem.at[COLUMN], spans[COLUMN])
        sums = cs_ref[pl.ds(pl.multiple_of(me_s * group, 8), group), :]
        for slot in range(n_s - 1):
            sums = sums + cr_ref[slot * group : (slot + 1) * group, :]
        plan = sums[:lane_tiles] / total_scen
        rest = sums[lane_tiles : 2 * lane_tiles]
        term = (2.0 * penalty) * plan * ((penalty / 2.0) * total_scen * plan - rest)
        ns_ref[0:1, :] = square_row + jnp.sum(term, axis=0, keepdims=True)
        pg_ref[pl.ds(own, lane_tiles), :] = plan
        exchange(k + 1)
        for kind in (ZONE, COLUMN, PLAN, IMB, NEAR, FAR):
            wait_for(send_sem.at[kind], spans[kind])
        return carry

    lax.fori_loop(0, ITERS - 1, iteration, 0)

    leaving = [pltpu.make_async_copy(plan_ref, plan_out, out_sem.at[0])]
    leaving[0].start()
    shrink, pay, _ = scalars(step_of(ITERS - 1))
    for j in range(blocks):
        cap = cap_ref[:, columns(j)]
        lowest = 0.02 * cap
        highest = 0.98 * cap

        def finish(s, none):
            here = (scen_rows(s), columns(j))
            x_ref[here] = jnp.clip(x_ref[here] - res_ref[here] * shrink, lowest, highest)
            return none

        lax.fori_loop(0, scens, finish, 0, unroll=4)
        copy = pltpu.make_async_copy(
            x_ref.at[:, columns(j)], x_out.at[:, columns(j)], out_sem.at[1 + j]
        )
        copy.start()
        leaving.append(copy)
    prices_ref[...] += pay * imb_ref[...]
    copy = pltpu.make_async_copy(prices_ref, prices_out, out_sem.at[1 + blocks])
    copy.start()
    leaving.append(copy)
    for copy in leaving:
        copy.wait()


def solution(mesh):
    n_s, n_g = mesh.shape["scen"], mesh.shape["gen"]
    scen_dims = (n_s // 2, 2)
    gen_dims = (2, n_g // 4, 2) if n_g >= 4 else (n_g, 1, 1)

    def local(
        zone_load,
        linear_cost,
        cost_diag,
        capacity,
        cost_tiles,
        coupling_tiles,
        block_map,
        zone_index,
        step_numer,
        step_denom,
    ):
        scens, periods, zones = zone_load.shape
        width = capacity.shape[0]
        blocks, tile, _ = cost_tiles.shape
        rows = scens * periods
        lane_tiles = width // LANES
        group = -(-(2 * lane_tiles) // 8) * 8
        plan_rows = -(-lane_tiles // 8) * 8
        entries = float(n_s * rows * width * n_g)
        zone_entries = float(n_s * rows * zones)
        hbm = pl.BlockSpec(memory_space=pltpu.HBM)
        state = pltpu.VMEM((rows, width), F32)
        share = rows // n_g
        dispatch, prices, plan = pl.pallas_call(
            functools.partial(
                kernel,
                scen_dims,
                gen_dims,
                entries,
                zone_entries,
                zones / (width * n_g),
            ),
            out_shape=(
                jax.ShapeDtypeStruct((rows, width), F32),
                jax.ShapeDtypeStruct((rows, zones), F32),
                jax.ShapeDtypeStruct((periods, width), F32),
            ),
            in_specs=[hbm] * 10,
            out_specs=(hbm, hbm, hbm),
            scratch_shapes=[
                state,
                pltpu.VMEM((rows, zones), F32),
                pltpu.VMEM((periods, width), F32),
                pltpu.VMEM((rows, zones), F32),
                pltpu.VMEM((periods, width), F32),
                pltpu.VMEM((width,), F32),
                pltpu.VMEM((width,), F32),
                pltpu.VMEM((blocks, tile, tile), BF16),
                pltpu.VMEM((blocks, tile, tile), BF16),
                pltpu.SMEM(block_map.shape, jnp.int32),
                pltpu.VMEM((width,), jnp.int32),
                pltpu.SMEM(step_numer.shape, jnp.int32),
                pltpu.SMEM(step_denom.shape, jnp.int32),
                state,
                state,
                state,
                state,
                pltpu.VMEM((zones, width), BF16),
                pltpu.VMEM((width, zones), BF16),
                pltpu.VMEM((blocks, tile, tile), BF16),
                pltpu.VMEM((1, width), F32),
                pltpu.VMEM((1, width), F32),
                pltpu.VMEM((periods, width), F32),
                pltpu.VMEM((periods, width), F32),
                pltpu.VMEM((periods, width), F32),
                pltpu.VMEM((periods, width), F32),
                pltpu.VMEM((periods, width), F32),
                pltpu.VMEM((n_g, 1, zones), F32),
                pltpu.VMEM((rows, zones), F32),
                pltpu.VMEM(((n_g - 1) * share, zones), F32),
                pltpu.VMEM((periods * group, LANES), F32),
                pltpu.VMEM(((n_s - 1) * group, LANES), F32),
                pltpu.VMEM((n_s * plan_rows, LANES), F32),
                pltpu.VMEM((rows, zones), F32),
                pltpu.VMEM((4, LANES), F32),
                pltpu.VMEM((scen_dims[0] - 1, 4, LANES), F32),
                pltpu.VMEM((4, LANES), F32),
                pltpu.VMEM((2, n_g * scen_dims[1] - 1, 4, LANES), F32),
                pltpu.VMEM((n_s - 1, 4, LANES), F32),
                pltpu.VMEM((4, LANES), F32),
                pltpu.SemaphoreType.DMA((8,)),
                pltpu.SemaphoreType.DMA((8,)),
                pltpu.SemaphoreType.DMA((2,)),
                pltpu.SemaphoreType.DMA((10,)),
                pltpu.SemaphoreType.DMA((cost_tiles.shape[0] + 2,)),
            ],
            compiler_params=pltpu.CompilerParams(collective_id=0, has_side_effects=True),
        )(
            zone_load.reshape(rows, zones),
            linear_cost,
            cost_diag,
            capacity,
            cost_tiles,
            coupling_tiles[0],
            block_map,
            zone_index,
            step_numer,
            step_denom,
        )
        return dispatch.reshape(scens, periods, width), prices.reshape(scens, periods, zones), plan

    return jax.shard_map(
        local,
        mesh=mesh,
        in_specs=(
            P("scen", None, None),
            P(None, "gen"),
            P("gen"),
            P("gen"),
            P("gen", None, None),
            P("scen", "gen", None, None),
            P("scen", "gen"),
            P("gen"),
            P(),
            P(),
        ),
        out_specs=(P("scen", None, "gen"), P("scen", None, None), P(None, "gen")),
        check_vma=False,
    )
```

```python
import functools
import itertools

import jax
import jax.numpy as jnp
from jax import lax
from jax.experimental import pallas as pl
from jax.experimental.pallas import tpu as pltpu
from jax.sharding import PartitionSpec as P

ITERS = 5
MESH = pl.DeviceIdType.MESH
F32 = jnp.float32
BF16 = jnp.bfloat16
LANES = 128

penalty = 2.0
centering = 0.5
epsilon = 1e-06


def ring(offset, size):
    return min(offset, size - offset)


def partners(dims, hops):
    result = []
    for offset in itertools.product(*[range(n) for n in dims]):
        if not any(offset):
            continue
        back = 0
        for o, n in zip(offset, dims):
            back = back * n + (n - o) % n
        result.append((hops(offset), offset, back - 1))
    result.sort(key=lambda item: -item[0])
    return [(offset, slot) for _, offset, slot in result]


def moved(me, dims, offset):
    index = 0
    stride = 1
    for n, o in zip(reversed(dims), reversed(offset)):
        coordinate = (me // stride) % n
        index = index + ((coordinate + o) % n) * stride
        stride *= n
    return index


def two_parts(value):
    high = value.astype(BF16)
    return high, (value - high.astype(F32)).astype(BF16)


def kernel(
    scen_dims,
    gen_dims,
    entries,
    zone_entries,
    zone_scale,
    load_hbm,
    linear_hbm,
    diag_hbm,
    cap_hbm,
    cost_hbm,
    coupling_hbm,
    map_hbm,
    zone_hbm,
    numer_hbm,
    denom_hbm,
    x_out,
    prices_out,
    plan_out,
    x_ref,
    prices_ref,
    plan_ref,
    load_ref,
    linear_ref,
    diag_in,
    cap_in,
    cost_ref,
    coupling_ref,
    map_ref,
    zone_in,
    numer_ref,
    denom_ref,
    low_ref,
    high_ref,
    res_ref,
    inv_ref,
    onehot_ref,
    turned_ref,
    masked_ref,
    diag_ref,
    cap_ref,
    column_ref,
    round_ref,
    dual_ref,
    paid_ref,
    more_ref,
    zc_ref,
    zp_ref,
    zr_ref,
    cs_ref,
    cr_ref,
    pg_ref,
    imb_ref,
    ns_ref,
    nr_ref,
    fs_ref,
    fr_ref,
    wide_ref,
    all_ref,
    send_sem,
    recv_sem,
    far_sem,
    in_sem,
    out_sem,
):
    me_s = lax.axis_index("scen")
    me_g = lax.axis_index("gen")
    depth, sides = scen_dims
    n_s = depth * sides
    n_g = gen_dims[0] * gen_dims[1] * gen_dims[2]
    y_hops = {(0, 0): 0, (0, 1): 1, (1, 0): 2, (1, 1): 1}

    def scen_device(offset):
        return {"scen": moved(me_s, scen_dims, offset)}

    def gen_device(offset):
        return {"gen": moved(me_g, gen_dims, offset)}

    def plane_device(offset):
        return {
            "scen": moved(me_s, scen_dims, (0, offset[0])),
            "gen": moved(me_g, gen_dims, offset[1:]),
        }

    scen_group = partners(scen_dims, lambda o: ring(o[0], depth) + 2 * o[1])
    gen_group = partners(gen_dims, lambda o: 2 * o[0] + 2 * ring(o[1], gen_dims[1]) + o[2])
    line_group = partners((depth,), lambda o: ring(o[0], depth))
    plane_group = partners(
        (sides,) + gen_dims,
        lambda o: 2 * y_hops[o[:2]] + 2 * ring(o[2], gen_dims[1]) + o[3],
    )
    scen_to = [(scen_device(o), moved(me_s, scen_dims, o), slot) for o, slot in scen_group]
    gen_to = [(gen_device(o), moved(me_g, gen_dims, o), slot) for o, slot in gen_group]
    line_to = [(scen_device((o[0], 0)), 0, slot) for o, slot in line_group]
    plane_to = [(plane_device(o), 0, slot) for o, slot in plane_group]

    barrier = pltpu.get_barrier_semaphore()
    greeted = [device for device, _, _ in scen_to]
    greeted += [plane_device(o) for o, _ in plane_group if any(o[1:])]
    for device in greeted:
        pl.semaphore_signal(barrier, inc=1, device_id=device, device_id_type=MESH)

    fetched = {}
    for position, (name, source, place) in enumerate(
        (
            ("zone", zone_hbm, zone_in),
            ("cap", cap_hbm, cap_in),
            ("diag", diag_hbm, diag_in),
            ("cost", cost_hbm, cost_ref),
            ("map", map_hbm, map_ref),
            ("coupling", coupling_hbm, coupling_ref),
            ("linear", linear_hbm, linear_ref),
            ("numer", numer_hbm, numer_ref),
            ("denom", denom_hbm, denom_ref),
            ("load", load_hbm, load_ref),
        )
    ):
        fetched[name] = pltpu.make_async_copy(source, place, in_sem.at[position])
        fetched[name].start()

    rows, width = x_ref.shape
    periods = plan_ref.shape[0]
    scens = rows // periods
    zones = zp_ref.shape[1]
    blocks, tile, _ = cost_ref.shape
    tiles = tile // LANES
    lane_tiles = width // LANES
    halves = periods // 8
    group = cs_ref.shape[0] // periods
    share = rows // n_g
    plan_rows = pg_ref.shape[0] // n_s
    total_scen = scens * n_s
    mine = pl.ds(pl.multiple_of(me_g * share, share), share)
    own = pl.multiple_of(me_s * plan_rows, plan_rows)

    def columns(j):
        return pl.ds(j * tile, tile)

    def scen_rows(s):
        return pl.ds(pl.multiple_of(s * periods, periods), periods)

    def send(kind, to, source, landing, sem=None):
        for device, member, slot in to:
            pltpu.make_async_remote_copy(
                src_ref=source(member),
                dst_ref=landing(slot),
                send_sem=send_sem.at[kind],
                recv_sem=recv_sem.at[kind] if sem is None else sem,
                device_id=device,
                device_id_type=MESH,
            ).start()

    def wait_for(sem, span):
        pltpu.make_async_copy(span, span, sem).wait()

    ZONE, COLUMN, PLAN, IMB, NEAR, FAR, START, WIDE = range(8)
    spans = {
        ZONE: zr_ref,
        COLUMN: cr_ref,
        PLAN: pg_ref.at[pl.ds(0, (n_s - 1) * plan_rows)],
        IMB: imb_ref.at[pl.ds(0, (n_g - 1) * share)],
        NEAR: nr_ref,
        FAR: fr_ref.at[0],
        START: zc_ref.at[pl.ds(0, n_g - 1)],
        WIDE: wide_ref,
    }

    def level(s, shape):
        ids = jnp.full(shape, me_s * scens + s, jnp.int32)
        return 0.2 + 0.6 * (ids.astype(F32) + 0.5) / total_scen

    def step_of(k):
        numer = jnp.full((1, 1), numer_ref[k], jnp.int32).astype(F32)
        return numer / jnp.full((1, 1), denom_ref[k], jnp.int32).astype(F32)

    def fold(value):
        row = jnp.sum(value, axis=0, keepdims=True)
        return sum(row[:, t * LANES : (t + 1) * LANES] for t in range(value.shape[1] // LANES))

    for name in ("zone", "cap", "diag"):
        fetched[name].wait()
    diag_ref[...] = diag_in[...].reshape(1, width)
    cap_ref[...] = cap_in[...].reshape(1, width)
    zone_row = zone_in[...].reshape(1, width)
    start = jnp.zeros((16, zones), F32)
    for j in range(blocks):
        ids = lax.broadcasted_iota(jnp.int32, (zones, tile), 0)
        onehot = jnp.where(ids == zone_row[:, j * tile : (j + 1) * tile], 1.0, 0.0)
        onehot_ref[:, columns(j)] = onehot.astype(BF16)
        turned = onehot.T.astype(BF16)
        turned_ref[columns(j), :] = turned
        cap_high, cap_low = two_parts(jnp.broadcast_to(cap_ref[:, columns(j)], (8, tile)))
        both = jnp.concatenate([cap_high, cap_low], axis=0)
        start = start + jnp.dot(both, turned, preferred_element_type=F32)
    zc_ref[me_g] = start[0:1] + start[8:9]

    for name in ("map", "coupling"):
        fetched[name].wait()
    for j in range(blocks):
        mask = map_ref[0, j].astype(F32)
        masked_ref[j] = (coupling_ref[j].astype(F32) * mask).astype(BF16)

    def begin(s, carry):
        here = scen_rows(s)
        x_ref[here, :] = level(s, (periods, width)) * cap_ref[...]
        low_ref[here, :] = jnp.ones((periods, width), F32)
        high_ref[here, :] = jnp.ones((periods, width), F32)
        return carry

    lax.fori_loop(0, scens, begin, 0, unroll=2)
    prices_ref[...] = jnp.zeros_like(prices_ref)
    paid_ref[...] = jnp.zeros_like(paid_ref)
    cs_ref[...] = jnp.zeros_like(cs_ref)
    ns_ref[...] = jnp.zeros_like(ns_ref)
    fs_ref[...] = jnp.zeros_like(fs_ref)
    pg_ref[...] = jnp.zeros_like(pg_ref)

    def residuals(step, first):
        if not first:
            price_high, price_low = two_parts(prices_ref[...])
        gap_row = jnp.zeros((1, LANES), F32)
        square_row = jnp.zeros((1, LANES), F32)
        keep = 1.0 - step
        for j in range(blocks):
            left = x_ref[:, columns(j)].astype(BF16)
            found = jnp.dot(left, cost_ref[j], preferred_element_type=F32) + jnp.dot(
                left, masked_ref[j], preferred_element_type=F32
            )
            if not first:
                onehot = onehot_ref[:, columns(j)]
                found = (
                    found
                    + jnp.dot(price_high, onehot, preferred_element_type=F32)
                    + jnp.dot(price_low, onehot, preferred_element_type=F32)
                )
            res_ref[:, columns(j)] = found
            cap = cap_ref[:, columns(j)]
            weight = diag_ref[:, columns(j)] + penalty
            fixed = linear_ref[:, columns(j)]
            if first:
                fixed = fixed - penalty * 0.5 * cap

            def part(s, sums):
                gap, square = sums
                here = (scen_rows(s), columns(j))
                value = x_ref[here]
                low = low_ref[here]
                high = high_ref[here]
                rest = cap - value
                residual = res_ref[here] + weight * value + fixed - low + high
                scale = step / (weight + low / value + high / rest)
                if first:
                    res_ref[here] = residual * scale
                else:
                    res_ref[here] = residual
                    inv_ref[here] = scale
                low_ref[here] = keep * low
                high_ref[here] = keep * high
                return gap + (value * low + rest * high), square + residual * residual

            zero = jnp.zeros((periods, tile), F32)
            gap, square = lax.fori_loop(0, scens, part, (zero, zero), unroll=2)
            gap_row = gap_row + fold(gap)
            square_row = square_row + fold(square)
        return gap_row, square_row

    def lump():
        lumped = jnp.zeros((periods, zones), F32)
        for s in range(scens):
            lumped = lumped + imb_ref[s * periods : (s + 1) * periods, :]
        both = jnp.concatenate(two_parts(lumped), axis=0)
        for j in range(blocks):
            found = jnp.dot(both, onehot_ref[:, columns(j)], preferred_element_type=F32)
            more_ref[:, columns(j)] = found[:periods] + found[periods:]

    def keep_sums(every):
        all_ref[...] = jnp.broadcast_to(jnp.sum(every, axis=1, keepdims=True), (4, LANES))

    def exchange(k):
        send(NEAR, line_to, lambda t: ns_ref, lambda slot: nr_ref.at[slot])
        send(
            PLAN,
            scen_to,
            lambda t: pg_ref.at[pl.ds(own, plan_rows)],
            lambda slot: pg_ref.at[pl.ds(own, plan_rows)],
        )
        wait_for(recv_sem.at[NEAR], spans[NEAR])
        near = ns_ref[...]
        for slot in range(depth - 1):
            near = near + nr_ref[slot]
        fs_ref[...] = near
        turn = lax.rem(k, 2)
        send(
            FAR,
            plane_to,
            lambda t: fs_ref,
            lambda slot: fr_ref.at[turn, slot],
            far_sem.at[turn],
        )
        wait_for(recv_sem.at[IMB], spans[IMB])
        lump()
        wait_for(recv_sem.at[PLAN], spans[PLAN])
        for j in range(blocks):
            pieces = [
                jnp.concatenate(
                    [
                        pg_ref[
                            pl.ds(h * 8 * plan_rows + j * tiles + t, 8, stride=plan_rows), :
                        ]
                        for t in range(tiles)
                    ],
                    axis=1,
                )
                for h in range(halves)
            ]
            plan = jnp.concatenate(pieces, axis=0)
            plan_ref[:, columns(j)] = plan
            twice = penalty * plan

            def settle(s, none):
                here = (scen_rows(s), columns(j))
                res_ref[here] = (res_ref[here] - twice) * inv_ref[here]
                return none

            lax.fori_loop(0, scens, settle, 0, unroll=4)
        wait_for(far_sem.at[turn], spans[FAR])
        every = fs_ref[...]
        for slot in range(n_g * sides - 1):
            every = every + fr_ref[turn, slot]
        keep_sums(every)

    def scalars(step):
        every = all_ref[:, 0:1]
        dual_rms = jnp.sqrt(every[0:1] / entries + epsilon)
        primal_rms = jnp.sqrt(every[1:2] / zone_entries + epsilon)
        target = centering * every[2:3] / (2.0 * entries)
        return 1.0 / (1.0 + dual_rms), step / (1.0 + primal_rms), step * target

    for name in ("numer", "denom", "linear", "cost"):
        fetched[name].wait()
    step = step_of(0)
    gap_row, square_row = residuals(step, True)
    fs_ref[0:1, :] = square_row
    fs_ref[2:3, :] = gap_row
    pl.semaphore_wait(barrier, len(greeted))
    send(START, gen_to, lambda t: zc_ref.at[me_g], lambda slot: zc_ref.at[me_g])
    send(FAR, plane_to, lambda t: fs_ref, lambda slot: fr_ref.at[0, slot], far_sem.at[0])
    fetched["load"].wait()
    wait_for(recv_sem.at[START], spans[START])
    per_zone = jnp.sum(zc_ref[...], axis=0)

    def imbalances(s, square):
        here = scen_rows(s)
        value = level(s, (periods, zones)) * per_zone * zone_scale - load_ref[here, :]
        imb_ref[here, :] = value
        return square + value * value

    square = lax.fori_loop(0, scens, imbalances, jnp.zeros((periods, zones), F32), unroll=2)
    primal_row = fold(square)
    wait_for(far_sem.at[0], spans[FAR])
    every = fs_ref[...]
    for slot in range(n_g * sides - 1):
        every = every + fr_ref[0, slot]
    ns_ref[...] = every * (1.0 / sides)
    ns_ref[1:2, :] = primal_row
    send(WIDE, scen_to, lambda t: ns_ref, lambda slot: wide_ref.at[slot])
    lump()
    wait_for(recv_sem.at[WIDE], spans[WIDE])
    every = ns_ref[...]
    for slot in range(n_s - 1):
        every = every + wide_ref[slot]
    keep_sums(every)
    for kind in (START, FAR, WIDE):
        wait_for(send_sem.at[kind], spans[kind])

    def iteration(k, carry):
        step = step_of(k)
        shrink, pay, pull = scalars(step)

        for j in range(blocks):
            cap = cap_ref[:, columns(j)]
            lowest = 0.02 * cap
            highest = 0.98 * cap

            def update(s, sums):
                column, rounded, dual = sums
                here = (scen_rows(s), columns(j))
                value = jnp.clip(x_ref[here] - res_ref[here] * shrink, lowest, highest)
                low = low_ref[here] + pull / value
                high = high_ref[here] + pull / (cap - value)
                x_ref[here] = value
                low_ref[here] = low
                high_ref[here] = high
                return (
                    column + value,
                    rounded + value.astype(BF16).astype(F32),
                    dual + (high - low),
                )

            zero = jnp.zeros((periods, tile), F32)
            column, rounded, dual = lax.fori_loop(
                0, scens, update, (zero, zero, zero), unroll=4
            )
            column_ref[:, columns(j)] = column
            round_ref[:, columns(j)] = rounded
            dual_ref[:, columns(j)] = dual

        for j in range(blocks):
            both = jnp.concatenate(two_parts(round_ref[:, columns(j)]), axis=0)
            found = jnp.dot(both, cost_ref[j], preferred_element_type=F32) + jnp.dot(
                both, masked_ref[j], preferred_element_type=F32
            )
            paid = paid_ref[:, columns(j)] + pay * more_ref[:, columns(j)]
            paid_ref[:, columns(j)] = paid
            column = column_ref[:, columns(j)]
            rest = (
                (found[:periods] + found[periods:])
                + (diag_ref[:, columns(j)] + penalty) * column
                + float(scens) * linear_ref[:, columns(j)]
                + paid
                + dual_ref[:, columns(j)]
            )
            for t in range(tiles):
                lanes = slice(t * LANES, (t + 1) * LANES)
                for h in range(halves):
                    first = h * 8 * group + j * tiles + t
                    cs_ref[pl.ds(first, 8, stride=group), :] = column[h * 8 : h * 8 + 8, lanes]
                    cs_ref[pl.ds(first + lane_tiles, 8, stride=group), :] = rest[
                        h * 8 : h * 8 + 8, lanes
                    ]
        send(
            COLUMN,
            scen_to,
            lambda t: cs_ref.at[pl.ds(t * group, group)],
            lambda slot: cr_ref.at[pl.ds(slot * group, group)],
        )
        prices_ref[...] += pay * imb_ref[...]

        found = None
        for j in range(blocks):
            for piece in two_parts(x_ref[:, columns(j)]):
                term = jnp.dot(piece, turned_ref[columns(j), :], preferred_element_type=F32)
                found = term if found is None else found + term
        zp_ref[...] = found
        send(
            ZONE,
            gen_to,
            lambda t: zp_ref.at[pl.ds(t * share, share)],
            lambda slot: zr_ref.at[pl.ds(slot * share, share)],
        )

        gap_row, square_row = residuals(step_of(k + 1), False)

        wait_for(recv_sem.at[ZONE], spans[ZONE])
        total = zp_ref[mine, :]
        for slot in range(n_g - 1):
            total = total + zr_ref[slot * share : (slot + 1) * share, :]
        imbalance = total * zone_scale - load_ref[mine, :]
        imb_ref[mine, :] = imbalance
        send(IMB, gen_to, lambda t: imb_ref.at[mine], lambda slot: imb_ref.at[mine])
        ns_ref[1:2, :] = fold(imbalance * imbalance)
        ns_ref[2:3, :] = gap_row

        wait_for(recv_sem.at[COLUMN], spans[COLUMN])
        sums = cs_ref[pl.ds(pl.multiple_of(me_s * group, 8), group), :]
        for slot in range(n_s - 1):
            sums = sums + cr_ref[slot * group : (slot + 1) * group, :]
        plan = sums[:lane_tiles] / total_scen
        rest = sums[lane_tiles : 2 * lane_tiles]
        term = (2.0 * penalty) * plan * ((penalty / 2.0) * total_scen * plan - rest)
        ns_ref[0:1, :] = square_row + jnp.sum(term, axis=0, keepdims=True)
        pg_ref[pl.ds(own, lane_tiles), :] = plan
        exchange(k + 1)
        for kind in (ZONE, COLUMN, PLAN, IMB, NEAR, FAR):
            wait_for(send_sem.at[kind], spans[kind])
        return carry

    lax.fori_loop(0, ITERS - 1, iteration, 0)

    leaving = [pltpu.make_async_copy(plan_ref, plan_out, out_sem.at[0])]
    leaving[0].start()
    shrink, pay, _ = scalars(step_of(ITERS - 1))
    for j in range(blocks):
        cap = cap_ref[:, columns(j)]
        lowest = 0.02 * cap
        highest = 0.98 * cap

        def finish(s, none):
            here = (scen_rows(s), columns(j))
            x_ref[here] = jnp.clip(x_ref[here] - res_ref[here] * shrink, lowest, highest)
            return none

        lax.fori_loop(0, scens, finish, 0, unroll=4)
        copy = pltpu.make_async_copy(
            x_ref.at[:, columns(j)], x_out.at[:, columns(j)], out_sem.at[1 + j]
        )
        copy.start()
        leaving.append(copy)
    prices_ref[...] += pay * imb_ref[...]
    copy = pltpu.make_async_copy(prices_ref, prices_out, out_sem.at[1 + blocks])
    copy.start()
    leaving.append(copy)
    for copy in leaving:
        copy.wait()


def relay(x_in, prices_in, plan_in, x_out, prices_out, plan_out, x, prices, plan, came, went):
    pieces = []
    rows = x.shape[0] // 4
    for part in range(4):
        here = pl.ds(part * rows, rows)
        pieces.append((x_in.at[here], x.at[here], x_out.at[here]))
    pieces.append((prices_in, prices, prices_out))
    pieces.append((plan_in, plan, plan_out))
    coming = [
        pltpu.make_async_copy(source, held, came.at[i]) for i, (source, held, _) in enumerate(pieces)
    ]
    going = [
        pltpu.make_async_copy(held, place, went.at[i]) for i, (_, held, place) in enumerate(pieces)
    ]
    for copy in coming:
        copy.start()
    for first, second in zip(coming, going):
        first.wait()
        second.start()
    for copy in going:
        copy.wait()


def solution(mesh):
    n_s, n_g = mesh.shape["scen"], mesh.shape["gen"]
    scen_dims = (n_s // 2, 2)
    gen_dims = (2, n_g // 4, 2) if n_g >= 4 else (n_g, 1, 1)

    def local(
        zone_load,
        linear_cost,
        cost_diag,
        capacity,
        cost_tiles,
        coupling_tiles,
        block_map,
        zone_index,
        step_numer,
        step_denom,
    ):
        scens, periods, zones = zone_load.shape
        width = capacity.shape[0]
        blocks, tile, _ = cost_tiles.shape
        rows = scens * periods
        lane_tiles = width // LANES
        group = -(-(2 * lane_tiles) // 8) * 8
        plan_rows = -(-lane_tiles // 8) * 8
        entries = float(n_s * rows * width * n_g)
        zone_entries = float(n_s * rows * zones)
        hbm = pl.BlockSpec(memory_space=pltpu.HBM)
        state = pltpu.VMEM((rows, width), F32)
        share = rows // n_g
        dispatch, prices, plan = pl.pallas_call(
            functools.partial(
                kernel,
                scen_dims,
                gen_dims,
                entries,
                zone_entries,
                zones / (width * n_g),
            ),
            out_shape=(
                jax.ShapeDtypeStruct((rows, width), F32),
                jax.ShapeDtypeStruct((rows, zones), F32),
                jax.ShapeDtypeStruct((periods, width), F32),
            ),
            in_specs=[hbm] * 10,
            out_specs=(hbm, hbm, hbm),
            scratch_shapes=[
                state,
                pltpu.VMEM((rows, zones), F32),
                pltpu.VMEM((periods, width), F32),
                pltpu.VMEM((rows, zones), F32),
                pltpu.VMEM((periods, width), F32),
                pltpu.VMEM((width,), F32),
                pltpu.VMEM((width,), F32),
                pltpu.VMEM((blocks, tile, tile), BF16),
                pltpu.VMEM((blocks, tile, tile), BF16),
                pltpu.SMEM(block_map.shape, jnp.int32),
                pltpu.VMEM((width,), jnp.int32),
                pltpu.SMEM(step_numer.shape, jnp.int32),
                pltpu.SMEM(step_denom.shape, jnp.int32),
                state,
                state,
                state,
                state,
                pltpu.VMEM((zones, width), BF16),
                pltpu.VMEM((width, zones), BF16),
                pltpu.VMEM((blocks, tile, tile), BF16),
                pltpu.VMEM((1, width), F32),
                pltpu.VMEM((1, width), F32),
                pltpu.VMEM((periods, width), F32),
                pltpu.VMEM((periods, width), F32),
                pltpu.VMEM((periods, width), F32),
                pltpu.VMEM((periods, width), F32),
                pltpu.VMEM((periods, width), F32),
                pltpu.VMEM((n_g, 1, zones), F32),
                pltpu.VMEM((rows, zones), F32),
                pltpu.VMEM(((n_g - 1) * share, zones), F32),
                pltpu.VMEM((periods * group, LANES), F32),
                pltpu.VMEM(((n_s - 1) * group, LANES), F32),
                pltpu.VMEM((n_s * plan_rows, LANES), F32),
                pltpu.VMEM((rows, zones), F32),
                pltpu.VMEM((4, LANES), F32),
                pltpu.VMEM((scen_dims[0] - 1, 4, LANES), F32),
                pltpu.VMEM((4, LANES), F32),
                pltpu.VMEM((2, n_g * scen_dims[1] - 1, 4, LANES), F32),
                pltpu.VMEM((n_s - 1, 4, LANES), F32),
                pltpu.VMEM((4, LANES), F32),
                pltpu.SemaphoreType.DMA((8,)),
                pltpu.SemaphoreType.DMA((8,)),
                pltpu.SemaphoreType.DMA((2,)),
                pltpu.SemaphoreType.DMA((10,)),
                pltpu.SemaphoreType.DMA((cost_tiles.shape[0] + 2,)),
            ],
            compiler_params=pltpu.CompilerParams(collective_id=0, has_side_effects=True),
        )(
            zone_load.reshape(rows, zones),
            linear_cost,
            cost_diag,
            capacity,
            cost_tiles,
            coupling_tiles[0],
            block_map,
            zone_index,
            step_numer,
            step_denom,
        )
        results = (dispatch, prices, plan)
        dispatch, prices, plan = pl.pallas_call(
            relay,
            out_shape=tuple(jax.ShapeDtypeStruct(r.shape, r.dtype) for r in results),
            in_specs=[hbm] * 3,
            out_specs=(hbm, hbm, hbm),
            scratch_shapes=[pltpu.VMEM(r.shape, r.dtype) for r in results]
            + [pltpu.SemaphoreType.DMA((6,)), pltpu.SemaphoreType.DMA((6,))],
        )(*results)
        return dispatch.reshape(scens, periods, width), prices.reshape(scens, periods, zones), plan

    return jax.shard_map(
        local,
        mesh=mesh,
        in_specs=(
            P("scen", None, None),
            P(None, "gen"),
            P("gen"),
            P("gen"),
            P("gen", None, None),
            P("scen", "gen", None, None),
            P("scen", "gen"),
            P("gen"),
            P(),
            P(),
        ),
        out_specs=(P("scen", None, "gen"), P("scen", None, None), P(None, "gen")),
        check_vma=False,
    )
```

```python
import functools
import itertools

import jax
import jax.numpy as jnp
from jax import lax
from jax.experimental import pallas as pl
from jax.experimental.pallas import tpu as pltpu
from jax.sharding import PartitionSpec as P

ITERS = 5
MESH = pl.DeviceIdType.MESH
F32 = jnp.float32
BF16 = jnp.bfloat16
LANES = 128

penalty = 2.0
centering = 0.5
epsilon = 1e-06


def ring(offset, size):
    return min(offset, size - offset)


def partners(dims, hops):
    result = []
    for offset in itertools.product(*[range(n) for n in dims]):
        if not any(offset):
            continue
        back = 0
        for o, n in zip(offset, dims):
            back = back * n + (n - o) % n
        result.append((hops(offset), offset, back - 1))
    result.sort(key=lambda item: -item[0])
    return [(offset, slot) for _, offset, slot in result]


def moved(me, dims, offset):
    index = 0
    stride = 1
    for n, o in zip(reversed(dims), reversed(offset)):
        coordinate = (me // stride) % n
        index = index + ((coordinate + o) % n) * stride
        stride *= n
    return index


def two_parts(value):
    high = value.astype(BF16)
    return high, (value - high.astype(F32)).astype(BF16)


def rates(every, step, entries, zone_entries):
    dual_rms = jnp.sqrt(every[0:1] / entries + epsilon)
    primal_rms = jnp.sqrt(every[1:2] / zone_entries + epsilon)
    target = centering * every[2:3] / (2.0 * entries)
    return 1.0 / (1.0 + dual_rms), step / (1.0 + primal_rms), step * target


def kernel(
    scen_dims,
    gen_dims,
    entries,
    zone_entries,
    zone_scale,
    load_hbm,
    linear_hbm,
    diag_hbm,
    cap_hbm,
    cost_hbm,
    coupling_hbm,
    map_hbm,
    zone_hbm,
    numer_hbm,
    denom_hbm,
    x_out,
    move_out,
    prices_out,
    imb_out,
    plan_out,
    all_out,
    x_ref,
    prices_ref,
    plan_ref,
    load_ref,
    linear_ref,
    diag_in,
    cap_in,
    cost_ref,
    coupling_ref,
    map_ref,
    zone_in,
    numer_ref,
    denom_ref,
    low_ref,
    high_ref,
    res_ref,
    inv_ref,
    onehot_ref,
    turned_ref,
    masked_ref,
    diag_ref,
    cap_ref,
    column_ref,
    round_ref,
    dual_ref,
    paid_ref,
    more_ref,
    zc_ref,
    zp_ref,
    zr_ref,
    cs_ref,
    cr_ref,
    pg_ref,
    imb_ref,
    ns_ref,
    nr_ref,
    fs_ref,
    fr_ref,
    wide_ref,
    all_ref,
    send_sem,
    recv_sem,
    far_sem,
    in_sem,
    out_sem,
):
    me_s = lax.axis_index("scen")
    me_g = lax.axis_index("gen")
    depth, sides = scen_dims
    n_s = depth * sides
    n_g = gen_dims[0] * gen_dims[1] * gen_dims[2]
    y_hops = {(0, 0): 0, (0, 1): 1, (1, 0): 2, (1, 1): 1}

    def scen_device(offset):
        return {"scen": moved(me_s, scen_dims, offset)}

    def gen_device(offset):
        return {"gen": moved(me_g, gen_dims, offset)}

    def plane_device(offset):
        return {
            "scen": moved(me_s, scen_dims, (0, offset[0])),
            "gen": moved(me_g, gen_dims, offset[1:]),
        }

    scen_group = partners(scen_dims, lambda o: ring(o[0], depth) + 2 * o[1])
    gen_group = partners(gen_dims, lambda o: 2 * o[0] + 2 * ring(o[1], gen_dims[1]) + o[2])
    line_group = partners((depth,), lambda o: ring(o[0], depth))
    plane_group = partners(
        (sides,) + gen_dims,
        lambda o: 2 * y_hops[o[:2]] + 2 * ring(o[2], gen_dims[1]) + o[3],
    )
    scen_to = [(scen_device(o), moved(me_s, scen_dims, o), slot) for o, slot in scen_group]
    gen_to = [(gen_device(o), moved(me_g, gen_dims, o), slot) for o, slot in gen_group]
    line_to = [(scen_device((o[0], 0)), 0, slot) for o, slot in line_group]
    plane_to = [(plane_device(o), 0, slot) for o, slot in plane_group]

    barrier = pltpu.get_barrier_semaphore()
    greeted = [device for device, _, _ in scen_to]
    greeted += [plane_device(o) for o, _ in plane_group if any(o[1:])]
    for device in greeted:
        pl.semaphore_signal(barrier, inc=1, device_id=device, device_id_type=MESH)

    fetched = {}
    for position, (name, source, place) in enumerate(
        (
            ("zone", zone_hbm, zone_in),
            ("cap", cap_hbm, cap_in),
            ("diag", diag_hbm, diag_in),
            ("cost", cost_hbm, cost_ref),
            ("map", map_hbm, map_ref),
            ("coupling", coupling_hbm, coupling_ref),
            ("linear", linear_hbm, linear_ref),
            ("numer", numer_hbm, numer_ref),
            ("denom", denom_hbm, denom_ref),
            ("load", load_hbm, load_ref),
        )
    ):
        fetched[name] = pltpu.make_async_copy(source, place, in_sem.at[position])
        fetched[name].start()

    rows, width = x_ref.shape
    periods = plan_ref.shape[0]
    scens = rows // periods
    zones = zp_ref.shape[1]
    blocks, tile, _ = cost_ref.shape
    tiles = tile // LANES
    lane_tiles = width // LANES
    halves = periods // 8
    group = cs_ref.shape[0] // periods
    share = rows // n_g
    plan_rows = pg_ref.shape[0] // n_s
    total_scen = scens * n_s
    mine = pl.ds(pl.multiple_of(me_g * share, share), share)
    own = pl.multiple_of(me_s * plan_rows, plan_rows)

    def columns(j):
        return pl.ds(j * tile, tile)

    def scen_rows(s):
        return pl.ds(pl.multiple_of(s * periods, periods), periods)

    def send(kind, to, source, landing, sem=None):
        for device, member, slot in to:
            pltpu.make_async_remote_copy(
                src_ref=source(member),
                dst_ref=landing(slot),
                send_sem=send_sem.at[kind],
                recv_sem=recv_sem.at[kind] if sem is None else sem,
                device_id=device,
                device_id_type=MESH,
            ).start()

    def wait_for(sem, span):
        pltpu.make_async_copy(span, span, sem).wait()

    ZONE, COLUMN, PLAN, IMB, NEAR, FAR, START, WIDE = range(8)
    spans = {
        ZONE: zr_ref,
        COLUMN: cr_ref,
        PLAN: pg_ref.at[pl.ds(0, (n_s - 1) * plan_rows)],
        IMB: imb_ref.at[pl.ds(0, (n_g - 1) * share)],
        NEAR: nr_ref,
        FAR: fr_ref.at[0],
        START: zc_ref.at[pl.ds(0, n_g - 1)],
        WIDE: wide_ref,
    }

    def level(s, shape):
        ids = jnp.full(shape, me_s * scens + s, jnp.int32)
        return 0.2 + 0.6 * (ids.astype(F32) + 0.5) / total_scen

    def step_of(k):
        numer = jnp.full((1, 1), numer_ref[k], jnp.int32).astype(F32)
        return numer / jnp.full((1, 1), denom_ref[k], jnp.int32).astype(F32)

    def fold(value):
        row = jnp.sum(value, axis=0, keepdims=True)
        return sum(row[:, t * LANES : (t + 1) * LANES] for t in range(value.shape[1] // LANES))

    for name in ("zone", "cap", "diag"):
        fetched[name].wait()
    diag_ref[...] = diag_in[...].reshape(1, width)
    cap_ref[...] = cap_in[...].reshape(1, width)
    zone_row = zone_in[...].reshape(1, width)
    start = jnp.zeros((16, zones), F32)
    for j in range(blocks):
        ids = lax.broadcasted_iota(jnp.int32, (zones, tile), 0)
        onehot = jnp.where(ids == zone_row[:, j * tile : (j + 1) * tile], 1.0, 0.0)
        onehot_ref[:, columns(j)] = onehot.astype(BF16)
        turned = onehot.T.astype(BF16)
        turned_ref[columns(j), :] = turned
        cap_high, cap_low = two_parts(jnp.broadcast_to(cap_ref[:, columns(j)], (8, tile)))
        both = jnp.concatenate([cap_high, cap_low], axis=0)
        start = start + jnp.dot(both, turned, preferred_element_type=F32)
    zc_ref[me_g] = start[0:1] + start[8:9]

    for name in ("map", "coupling"):
        fetched[name].wait()
    for j in range(blocks):
        mask = map_ref[0, j].astype(F32)
        masked_ref[j] = (coupling_ref[j].astype(F32) * mask).astype(BF16)

    def begin(s, carry):
        here = scen_rows(s)
        x_ref[here, :] = level(s, (periods, width)) * cap_ref[...]
        low_ref[here, :] = jnp.ones((periods, width), F32)
        high_ref[here, :] = jnp.ones((periods, width), F32)
        return carry

    lax.fori_loop(0, scens, begin, 0, unroll=2)
    prices_ref[...] = jnp.zeros_like(prices_ref)
    paid_ref[...] = jnp.zeros_like(paid_ref)
    cs_ref[...] = jnp.zeros_like(cs_ref)
    ns_ref[...] = jnp.zeros_like(ns_ref)
    fs_ref[...] = jnp.zeros_like(fs_ref)
    pg_ref[...] = jnp.zeros_like(pg_ref)

    def residuals(step, first):
        if not first:
            price_high, price_low = two_parts(prices_ref[...])
        gap_row = jnp.zeros((1, LANES), F32)
        square_row = jnp.zeros((1, LANES), F32)
        keep = 1.0 - step
        for j in range(blocks):
            left = x_ref[:, columns(j)].astype(BF16)
            found = jnp.dot(left, cost_ref[j], preferred_element_type=F32) + jnp.dot(
                left, masked_ref[j], preferred_element_type=F32
            )
            if not first:
                onehot = onehot_ref[:, columns(j)]
                found = (
                    found
                    + jnp.dot(price_high, onehot, preferred_element_type=F32)
                    + jnp.dot(price_low, onehot, preferred_element_type=F32)
                )
            res_ref[:, columns(j)] = found
            cap = cap_ref[:, columns(j)]
            weight = diag_ref[:, columns(j)] + penalty
            fixed = linear_ref[:, columns(j)]
            if first:
                fixed = fixed - penalty * 0.5 * cap

            def part(s, sums):
                gap, square = sums
                here = (scen_rows(s), columns(j))
                value = x_ref[here]
                low = low_ref[here]
                high = high_ref[here]
                rest = cap - value
                residual = res_ref[here] + weight * value + fixed - low + high
                scale = step / (weight + low / value + high / rest)
                if first:
                    res_ref[here] = residual * scale
                else:
                    res_ref[here] = residual
                    inv_ref[here] = scale
                low_ref[here] = keep * low
                high_ref[here] = keep * high
                return gap + (value * low + rest * high), square + residual * residual

            zero = jnp.zeros((periods, tile), F32)
            gap, square = lax.fori_loop(0, scens, part, (zero, zero), unroll=2)
            gap_row = gap_row + fold(gap)
            square_row = square_row + fold(square)
        return gap_row, square_row

    def lump():
        lumped = jnp.zeros((periods, zones), F32)
        for s in range(scens):
            lumped = lumped + imb_ref[s * periods : (s + 1) * periods, :]
        both = jnp.concatenate(two_parts(lumped), axis=0)
        for j in range(blocks):
            found = jnp.dot(both, onehot_ref[:, columns(j)], preferred_element_type=F32)
            more_ref[:, columns(j)] = found[:periods] + found[periods:]

    def keep_sums(every):
        all_ref[...] = jnp.broadcast_to(jnp.sum(every, axis=1, keepdims=True), (4, LANES))

    def exchange(k):
        send(NEAR, line_to, lambda t: ns_ref, lambda slot: nr_ref.at[slot])
        send(
            PLAN,
            scen_to,
            lambda t: pg_ref.at[pl.ds(own, plan_rows)],
            lambda slot: pg_ref.at[pl.ds(own, plan_rows)],
        )
        wait_for(recv_sem.at[NEAR], spans[NEAR])
        near = ns_ref[...]
        for slot in range(depth - 1):
            near = near + nr_ref[slot]
        fs_ref[...] = near
        turn = lax.rem(k, 2)
        send(
            FAR,
            plane_to,
            lambda t: fs_ref,
            lambda slot: fr_ref.at[turn, slot],
            far_sem.at[turn],
        )
        wait_for(recv_sem.at[IMB], spans[IMB])
        lump()
        wait_for(recv_sem.at[PLAN], spans[PLAN])
        for j in range(blocks):
            pieces = [
                jnp.concatenate(
                    [
                        pg_ref[
                            pl.ds(h * 8 * plan_rows + j * tiles + t, 8, stride=plan_rows), :
                        ]
                        for t in range(tiles)
                    ],
                    axis=1,
                )
                for h in range(halves)
            ]
            plan = jnp.concatenate(pieces, axis=0)
            plan_ref[:, columns(j)] = plan
            twice = penalty * plan

            def settle(s, none):
                here = (scen_rows(s), columns(j))
                res_ref[here] = (res_ref[here] - twice) * inv_ref[here]
                return none

            lax.fori_loop(0, scens, settle, 0, unroll=4)
        leaving = [
            pltpu.make_async_copy(source, place, out_sem.at[i])
            for i, (source, place) in enumerate(
                (
                    (x_ref, x_out),
                    (res_ref, move_out),
                    (prices_ref, prices_out),
                    (imb_ref, imb_out),
                    (plan_ref, plan_out),
                )
            )
        ]
        for copy in leaving:
            copy.start()
        wait_for(far_sem.at[turn], spans[FAR])
        every = fs_ref[...]
        for slot in range(n_g * sides - 1):
            every = every + fr_ref[turn, slot]
        keep_sums(every)
        for copy in leaving:
            copy.wait()

    def scalars(step):
        return rates(all_ref[:, 0:1], step, entries, zone_entries)

    for name in ("numer", "denom", "linear", "cost"):
        fetched[name].wait()
    step = step_of(0)
    gap_row, square_row = residuals(step, True)
    fs_ref[0:1, :] = square_row
    fs_ref[2:3, :] = gap_row
    pl.semaphore_wait(barrier, len(greeted))
    send(START, gen_to, lambda t: zc_ref.at[me_g], lambda slot: zc_ref.at[me_g])
    send(FAR, plane_to, lambda t: fs_ref, lambda slot: fr_ref.at[0, slot], far_sem.at[0])
    fetched["load"].wait()
    wait_for(recv_sem.at[START], spans[START])
    per_zone = jnp.sum(zc_ref[...], axis=0)

    def imbalances(s, square):
        here = scen_rows(s)
        value = level(s, (periods, zones)) * per_zone * zone_scale - load_ref[here, :]
        imb_ref[here, :] = value
        return square + value * value

    square = lax.fori_loop(0, scens, imbalances, jnp.zeros((periods, zones), F32), unroll=2)
    primal_row = fold(square)
    wait_for(far_sem.at[0], spans[FAR])
    every = fs_ref[...]
    for slot in range(n_g * sides - 1):
        every = every + fr_ref[0, slot]
    ns_ref[...] = every * (1.0 / sides)
    ns_ref[1:2, :] = primal_row
    send(WIDE, scen_to, lambda t: ns_ref, lambda slot: wide_ref.at[slot])
    lump()
    wait_for(recv_sem.at[WIDE], spans[WIDE])
    every = ns_ref[...]
    for slot in range(n_s - 1):
        every = every + wide_ref[slot]
    keep_sums(every)
    for kind in (START, FAR, WIDE):
        wait_for(send_sem.at[kind], spans[kind])

    def iteration(k, carry):
        step = step_of(k)
        shrink, pay, pull = scalars(step)

        for j in range(blocks):
            cap = cap_ref[:, columns(j)]
            lowest = 0.02 * cap
            highest = 0.98 * cap

            def update(s, sums):
                column, rounded, dual = sums
                here = (scen_rows(s), columns(j))
                value = jnp.clip(x_ref[here] - res_ref[here] * shrink, lowest, highest)
                low = low_ref[here] + pull / value
                high = high_ref[here] + pull / (cap - value)
                x_ref[here] = value
                low_ref[here] = low
                high_ref[here] = high
                return (
                    column + value,
                    rounded + value.astype(BF16).astype(F32),
                    dual + (high - low),
                )

            zero = jnp.zeros((periods, tile), F32)
            column, rounded, dual = lax.fori_loop(
                0, scens, update, (zero, zero, zero), unroll=4
            )
            column_ref[:, columns(j)] = column
            round_ref[:, columns(j)] = rounded
            dual_ref[:, columns(j)] = dual

        for j in range(blocks):
            both = jnp.concatenate(two_parts(round_ref[:, columns(j)]), axis=0)
            found = jnp.dot(both, cost_ref[j], preferred_element_type=F32) + jnp.dot(
                both, masked_ref[j], preferred_element_type=F32
            )
            paid = paid_ref[:, columns(j)] + pay * more_ref[:, columns(j)]
            paid_ref[:, columns(j)] = paid
            column = column_ref[:, columns(j)]
            rest = (
                (found[:periods] + found[periods:])
                + (diag_ref[:, columns(j)] + penalty) * column
                + float(scens) * linear_ref[:, columns(j)]
                + paid
                + dual_ref[:, columns(j)]
            )
            for t in range(tiles):
                lanes = slice(t * LANES, (t + 1) * LANES)
                for h in range(halves):
                    first = h * 8 * group + j * tiles + t
                    cs_ref[pl.ds(first, 8, stride=group), :] = column[h * 8 : h * 8 + 8, lanes]
                    cs_ref[pl.ds(first + lane_tiles, 8, stride=group), :] = rest[
                        h * 8 : h * 8 + 8, lanes
                    ]
        send(
            COLUMN,
            scen_to,
            lambda t: cs_ref.at[pl.ds(t * group, group)],
            lambda slot: cr_ref.at[pl.ds(slot * group, group)],
        )
        prices_ref[...] += pay * imb_ref[...]

        found = None
        for j in range(blocks):
            for piece in two_parts(x_ref[:, columns(j)]):
                term = jnp.dot(piece, turned_ref[columns(j), :], preferred_element_type=F32)
                found = term if found is None else found + term
        zp_ref[...] = found
        send(
            ZONE,
            gen_to,
            lambda t: zp_ref.at[pl.ds(t * share, share)],
            lambda slot: zr_ref.at[pl.ds(slot * share, share)],
        )

        gap_row, square_row = residuals(step_of(k + 1), False)

        wait_for(recv_sem.at[ZONE], spans[ZONE])
        total = zp_ref[mine, :]
        for slot in range(n_g - 1):
            total = total + zr_ref[slot * share : (slot + 1) * share, :]
        imbalance = total * zone_scale - load_ref[mine, :]
        imb_ref[mine, :] = imbalance
        send(IMB, gen_to, lambda t: imb_ref.at[mine], lambda slot: imb_ref.at[mine])
        ns_ref[1:2, :] = fold(imbalance * imbalance)
        ns_ref[2:3, :] = gap_row

        wait_for(recv_sem.at[COLUMN], spans[COLUMN])
        sums = cs_ref[pl.ds(pl.multiple_of(me_s * group, 8), group), :]
        for slot in range(n_s - 1):
            sums = sums + cr_ref[slot * group : (slot + 1) * group, :]
        plan = sums[:lane_tiles] / total_scen
        rest = sums[lane_tiles : 2 * lane_tiles]
        term = (2.0 * penalty) * plan * ((penalty / 2.0) * total_scen * plan - rest)
        ns_ref[0:1, :] = square_row + jnp.sum(term, axis=0, keepdims=True)
        pg_ref[pl.ds(own, lane_tiles), :] = plan
        exchange(k + 1)
        for kind in (ZONE, COLUMN, PLAN, IMB, NEAR, FAR):
            wait_for(send_sem.at[kind], spans[kind])
        return carry

    lax.fori_loop(0, ITERS - 1, iteration, 0)

    copy = pltpu.make_async_copy(all_ref, all_out, out_sem.at[5])
    copy.start()
    copy.wait()


def finish(
    entries,
    zone_entries,
    last,
    x_in,
    move_in,
    prices_in,
    imb_in,
    plan_in,
    all_in,
    cap_in,
    numer_ref,
    denom_ref,
    x_out,
    prices_out,
    plan_out,
    x,
    move,
    prices,
    imb,
    plan,
    every,
    cap_flat,
    came,
    went,
):
    parts = 4
    rows = x.shape[0] // parts
    small = [(all_in, every), (cap_in, cap_flat)]
    for part in range(parts):
        here = pl.ds(part * rows, rows)
        small += [(x_in.at[here], x.at[here]), (move_in.at[here], move.at[here])]
    small += [(prices_in, prices), (imb_in, imb), (plan_in, plan)]
    coming = [pltpu.make_async_copy(a, b, came.at[i]) for i, (a, b) in enumerate(small)]
    for copy in coming:
        copy.start()
    coming[0].wait()
    coming[1].wait()
    numer = jnp.full((1, 1), numer_ref[last], jnp.int32).astype(F32)
    step = numer / jnp.full((1, 1), denom_ref[last], jnp.int32).astype(F32)
    shrink, pay, _ = rates(every[:, 0:1], step, entries, zone_entries)
    cap = cap_flat[...].reshape(1, x.shape[1])
    lowest = 0.02 * cap
    highest = 0.98 * cap
    going = []

    def leave(source, place):
        copy = pltpu.make_async_copy(source, place, went.at[len(going)])
        copy.start()
        going.append(copy)

    for part in range(parts):
        coming[2 + 2 * part].wait()
        coming[3 + 2 * part].wait()

        def clipped(i, none):
            here = pl.ds(pl.multiple_of(part * rows + i * 8, 8), 8)
            x[here, :] = jnp.clip(x[here, :] - move[here, :] * shrink, lowest, highest)
            return none

        lax.fori_loop(0, rows // 8, clipped, 0, unroll=2)
        here = pl.ds(part * rows, rows)
        leave(x.at[here], x_out.at[here])
    for copy in coming[2 + 2 * parts :]:
        copy.wait()
    leave(plan, plan_out)
    prices[...] += pay * imb[...]
    leave(prices, prices_out)
    for copy in going:
        copy.wait()


def solution(mesh):
    n_s, n_g = mesh.shape["scen"], mesh.shape["gen"]
    scen_dims = (n_s // 2, 2)
    gen_dims = (2, n_g // 4, 2) if n_g >= 4 else (n_g, 1, 1)

    def local(
        zone_load,
        linear_cost,
        cost_diag,
        capacity,
        cost_tiles,
        coupling_tiles,
        block_map,
        zone_index,
        step_numer,
        step_denom,
    ):
        scens, periods, zones = zone_load.shape
        width = capacity.shape[0]
        blocks, tile, _ = cost_tiles.shape
        rows = scens * periods
        lane_tiles = width // LANES
        group = -(-(2 * lane_tiles) // 8) * 8
        plan_rows = -(-lane_tiles // 8) * 8
        entries = float(n_s * rows * width * n_g)
        zone_entries = float(n_s * rows * zones)
        hbm = pl.BlockSpec(memory_space=pltpu.HBM)
        state = pltpu.VMEM((rows, width), F32)
        share = rows // n_g
        results = pl.pallas_call(
            functools.partial(
                kernel,
                scen_dims,
                gen_dims,
                entries,
                zone_entries,
                zones / (width * n_g),
            ),
            out_shape=(
                jax.ShapeDtypeStruct((rows, width), F32),
                jax.ShapeDtypeStruct((rows, width), F32),
                jax.ShapeDtypeStruct((rows, zones), F32),
                jax.ShapeDtypeStruct((rows, zones), F32),
                jax.ShapeDtypeStruct((periods, width), F32),
                jax.ShapeDtypeStruct((4, LANES), F32),
            ),
            in_specs=[hbm] * 10,
            out_specs=(hbm,) * 6,
            scratch_shapes=[
                state,
                pltpu.VMEM((rows, zones), F32),
                pltpu.VMEM((periods, width), F32),
                pltpu.VMEM((rows, zones), F32),
                pltpu.VMEM((periods, width), F32),
                pltpu.VMEM((width,), F32),
                pltpu.VMEM((width,), F32),
                pltpu.VMEM((blocks, tile, tile), BF16),
                pltpu.VMEM((blocks, tile, tile), BF16),
                pltpu.SMEM(block_map.shape, jnp.int32),
                pltpu.VMEM((width,), jnp.int32),
                pltpu.SMEM(step_numer.shape, jnp.int32),
                pltpu.SMEM(step_denom.shape, jnp.int32),
                state,
                state,
                state,
                state,
                pltpu.VMEM((zones, width), BF16),
                pltpu.VMEM((width, zones), BF16),
                pltpu.VMEM((blocks, tile, tile), BF16),
                pltpu.VMEM((1, width), F32),
                pltpu.VMEM((1, width), F32),
                pltpu.VMEM((periods, width), F32),
                pltpu.VMEM((periods, width), F32),
                pltpu.VMEM((periods, width), F32),
                pltpu.VMEM((periods, width), F32),
                pltpu.VMEM((periods, width), F32),
                pltpu.VMEM((n_g, 1, zones), F32),
                pltpu.VMEM((rows, zones), F32),
                pltpu.VMEM(((n_g - 1) * share, zones), F32),
                pltpu.VMEM((periods * group, LANES), F32),
                pltpu.VMEM(((n_s - 1) * group, LANES), F32),
                pltpu.VMEM((n_s * plan_rows, LANES), F32),
                pltpu.VMEM((rows, zones), F32),
                pltpu.VMEM((4, LANES), F32),
                pltpu.VMEM((scen_dims[0] - 1, 4, LANES), F32),
                pltpu.VMEM((4, LANES), F32),
                pltpu.VMEM((2, n_g * scen_dims[1] - 1, 4, LANES), F32),
                pltpu.VMEM((n_s - 1, 4, LANES), F32),
                pltpu.VMEM((4, LANES), F32),
                pltpu.SemaphoreType.DMA((8,)),
                pltpu.SemaphoreType.DMA((8,)),
                pltpu.SemaphoreType.DMA((2,)),
                pltpu.SemaphoreType.DMA((10,)),
                pltpu.SemaphoreType.DMA((6,)),
            ],
            compiler_params=pltpu.CompilerParams(collective_id=0, has_side_effects=True),
        )(
            zone_load.reshape(rows, zones),
            linear_cost,
            cost_diag,
            capacity,
            cost_tiles,
            coupling_tiles[0],
            block_map,
            zone_index,
            step_numer,
            step_denom,
        )
        smem = pl.BlockSpec(memory_space=pltpu.SMEM)
        dispatch, prices, plan = pl.pallas_call(
            functools.partial(finish, entries, zone_entries, ITERS - 1),
            out_shape=tuple(jax.ShapeDtypeStruct(results[i].shape, F32) for i in (0, 2, 4)),
            in_specs=[hbm] * 7 + [smem] * 2,
            out_specs=(hbm, hbm, hbm),
            scratch_shapes=[pltpu.VMEM(r.shape, r.dtype) for r in results]
            + [
                pltpu.VMEM((width,), F32),
                pltpu.SemaphoreType.DMA((13,)),
                pltpu.SemaphoreType.DMA((6,)),
            ],
        )(*results, capacity, step_numer, step_denom)
        return dispatch.reshape(scens, periods, width), prices.reshape(scens, periods, zones), plan

    return jax.shard_map(
        local,
        mesh=mesh,
        in_specs=(
            P("scen", None, None),
            P(None, "gen"),
            P("gen"),
            P("gen"),
            P("gen", None, None),
            P("scen", "gen", None, None),
            P("scen", "gen"),
            P("gen"),
            P(),
            P(),
        ),
        out_specs=(P("scen", None, "gen"), P("scen", None, None), P(None, "gen")),
        check_vma=False,
    )
```
